32 devices in a mesh: dp: 4 (over x, core), tensor: 8 (over z, y).
Axes of the slice: x: 2, y: 2, z: 4, core: 2. Of those that a mesh axis runs over, the one named last changes fastest.
Arguments:
- head_outputs: bfloat16 [4096, 4096], P('dp', 'tensor'), may hold values from -6 to 6
- out_weight: bfloat16 [4096, 4096], P('tensor'), may hold values from -0.09375 to 0.09375
- residual: bfloat16 [4096, 4096], P(('dp', 'tensor')), may hold values from -6 to 6
- norm_gain: float32 [4096], replicated, may hold values from 0.25 to 1.75
- chosen: int32 [16, 256], replicated, may hold values from 0 to 4095, as said below
- gates: float32 [16, 256], replicated, may hold values from 0.25 to 1
- place: int32 [16], replicated, may hold values from 0 to 15, each once
- w_gate: bfloat16 [32, 704, 4096], P(('dp', 'tensor')), may hold values from -0.09375 to 0.09375
- w_up: bfloat16 [32, 704, 4096], P(('dp', 'tensor')), may hold values from -0.09375 to 0.09375
- w_down: bfloat16 [32, 704, 4096], P(('dp', 'tensor')), may hold values from -0.15625 to 0.15625
Outputs:
- mixed: bfloat16 [4096, 4096], P(('dp', 'tensor'))
The draws below stay inside these ranges and needn't reach their ends.
Inputs may be any that keep to these rules, and one draw needn't show every extreme that they name: `chosen`: row e lists 256 different tokens; at most 16 of them lie in one aligned block of 128 rows (the rows of one device), and in every row some block holds exactly 16.
All inputs are finite; a program needn't handle non-finite values.
Results may differ from the reference program's by a relative error of at most 0.012.
Values may be sent and summed in bfloat16 or wider, within the bound.
A program may use at most 128 MiB of HBM per device.

```python
import jax
import jax.numpy as jnp
from jax import lax

D = 4096
HEADS = 32
HEAD_DIM = 128
FF = 1408
TOK_DEV = 128
OWNERS = 32
EXPERTS = 16
TOKENS = 4096
CAP = 256
MOST = 16
N_TENSOR = 8


def draw_chosen(key, part):
    keys = jax.random.split(key, 4)
    popularity = jax.random.randint(keys[0], (OWNERS,), 0, 3)
    noise = jax.random.randint(keys[1], (EXPERTS, OWNERS), 0, 64)
    device_ids = jnp.arange(OWNERS, dtype=jnp.int32)
    ranking = (noise + 32 * popularity[None, :]) * OWNERS + device_ids[None, :]
    _, order = lax.top_k(ranking, OWNERS)
    position = jnp.argsort(order, axis=1)
    quarter = OWNERS // 4
    counts = jnp.where(position < quarter, MOST, jnp.where(position < 3 * quarter, MOST // 2, 0))
    shuffle = jax.random.randint(keys[2], (EXPERTS, OWNERS, TOK_DEV), 0, 4096) * TOK_DEV + jnp.arange(TOK_DEV, dtype=jnp.int32)[None, None, :]
    picks = jnp.argsort(shuffle, axis=2)[:, :, :MOST].astype(jnp.int32)
    candidates = device_ids[None, :, None] * TOK_DEV + picks
    live = (jnp.arange(MOST, dtype=jnp.int32)[None, None, :] < counts[:, :, None]).astype(jnp.int32)
    spread = OWNERS * MOST
    order_key = jax.random.randint(keys[3], (EXPERTS, spread), 0, 4096) * spread + jnp.arange(spread, dtype=jnp.int32)[None, :]
    priority = live.reshape(EXPERTS, spread) * (4096 * spread) + order_key
    _, slots = lax.top_k(priority, CAP)
    return jnp.take_along_axis(candidates.reshape(EXPERTS, spread), slots, axis=1).astype(jnp.int32)


def levels(rng, shape, cuts, smallest, largest):
    def one(axis_at, parts):
        draws = jax.random.uniform(jax.random.fold_in(jax.random.fold_in(rng, 6), axis_at), (parts,), jnp.float32, smallest / len(cuts), largest / len(cuts))
        return jnp.repeat(jnp.exp(draws), shape[axis_at] // parts).reshape((-1,) + (1,) * (len(shape) - axis_at - 1))

    factor_of = one(*cuts[0])
    for cut in cuts[1:]:
        factor_of = factor_of * one(*cut)
    return factor_of


def bell_draw(own_key, shape, scale, bound, pieces=(), kind=jnp.bfloat16):
    array = scale * jax.random.normal(own_key, shape, jnp.float32)
    if pieces:
        array = array * levels(own_key, shape, pieces, -0.22, 0.18)
    return jnp.clip(array, -bound, bound).astype(kind)


def setup_inputs(seed: int = 0) -> dict:
    streams_of = jax.random.split(jax.random.key(seed), 11)
    return {
        "head_outputs": bell_draw(streams_of[0], (TOKENS, HEADS * HEAD_DIM), 1.0, 6.0, ((0, 4), (1, 8))),
        "out_weight": bell_draw(streams_of[1], (HEADS * HEAD_DIM, D), (HEADS * HEAD_DIM) ** -0.5, 0.09375, ((0, 8),)),
        "residual": bell_draw(streams_of[2], (TOKENS, D), 1.0, 6.0, ((0, 32),)),
        "norm_gain": jnp.clip(1.0 + 0.15 * jax.random.normal(streams_of[3], (D,), jnp.float32), 0.25, 1.75),
        "chosen": draw_chosen(jax.random.fold_in(streams_of[10], 71), 0),
        "gates": jnp.clip(jax.random.uniform(streams_of[5], (EXPERTS, CAP), jnp.float32, 0.25, 1.0), 0.25, 1.0),
        "place": jax.random.permutation(streams_of[6], EXPERTS).astype(jnp.int32),
        "w_gate": bell_draw(streams_of[7], (OWNERS, FF // 2, D), D ** -0.5, 0.09375, ((0, 32),)),
        "w_up": bell_draw(streams_of[8], (OWNERS, FF // 2, D), D ** -0.5, 0.09375, ((0, 32),)),
        "w_down": bell_draw(streams_of[9], (OWNERS, FF // 2, D), FF ** -0.5, 0.15625, ((0, 32),)),
    }


def rounded(value):
    return lax.optimization_barrier(value.astype(jnp.bfloat16)).astype(jnp.float32)

def reference(head_outputs, out_weight, residual, norm_gain, chosen, gates, place, w_gate, w_up, w_down):
    block_cols = head_outputs.shape[1] // N_TENSOR
    projected = jnp.zeros((head_outputs.shape[0], out_weight.shape[1]), jnp.float32)
    for block in range(N_TENSOR):
        left = head_outputs[:, block * block_cols:(block + 1) * block_cols]
        right = out_weight[block * block_cols:(block + 1) * block_cols]
        projected = projected + rounded(jnp.dot(left, right, preferred_element_type=jnp.float32))
    layer_state = residual.astype(jnp.float32) + projected
    scale = lax.rsqrt(lax.optimization_barrier(jnp.mean(layer_state * layer_state, axis=1, keepdims=True)) + 1.0)
    normed = (layer_state * scale * norm_gain.astype(jnp.float32)[None, :]).astype(jnp.bfloat16)
    contract = (((1,), (1,)), ((), ()))

    def expert_step(carry, inputs):
        token_rows, gate_row, slot = inputs
        inputs_rows = normed[token_rows]
        summed = jnp.zeros((token_rows.shape[0], normed.shape[1]), jnp.float32)
        for half in range(2):
            index = (2 * slot + half).astype(jnp.int32)
            gate_half = lax.dynamic_index_in_dim(w_gate, index, 0, keepdims=False)
            up_half = lax.dynamic_index_in_dim(w_up, index, 0, keepdims=False)
            down_half = lax.dynamic_index_in_dim(w_down, index, 0, keepdims=False)
            gate_part = lax.dot_general(inputs_rows, gate_half, contract, preferred_element_type=jnp.float32)
            up_part = lax.dot_general(inputs_rows, up_half, contract, preferred_element_type=jnp.float32)
            hidden = (jax.nn.silu(gate_part) * up_part).astype(jnp.bfloat16)
            half_out = jnp.dot(hidden, down_half, preferred_element_type=jnp.float32).astype(jnp.bfloat16)
            summed = summed + half_out.astype(jnp.float32)
        return (carry.at[token_rows].add(gate_row.astype(jnp.float32)[:, None] * summed), None)
    moe, _ = lax.scan(expert_step, jnp.zeros(layer_state.shape, jnp.float32), (chosen, gates, place))
    return (layer_state + moe).astype(jnp.bfloat16)
```

```python
import functools

import jax
import jax.numpy as jnp
from jax import lax
from jax.experimental import pallas as pl
from jax.experimental.pallas import tpu as pltpu
from jax.sharding import PartitionSpec as P

MESH = pl.DeviceIdType.MESH
LANES = 4
PIECES = 4
SEND_ORDER = (1, 2, 3, 0)
FORWARD_ORDER = (0, 2, 1, 3)
COMPUTE_ORDER = (2, 0, 3, 1)
EARLY = 2


def ring_rank(position, count):
    upper = position // (count // 2)
    return (1 - upper) * 2 * position + upper * (2 * (count - 1 - position) + 1)


def routing(place, chosen, gates, my_index, row_count, pick, gain_ref):
    experts, capacity = chosen.shape
    most = pick.shape[1]
    pair_ids = lax.broadcasted_iota(jnp.int32, (experts, experts), 0)
    pair_map = (place == pair_ids).astype(jnp.float32)
    chosen_pair = jnp.dot(
        pair_map,
        chosen.astype(jnp.float32),
        precision=lax.Precision.HIGHEST,
        preferred_element_type=jnp.float32,
    ).astype(jnp.int32)
    gates_pair = jnp.dot(
        pair_map, gates, precision=lax.Precision.HIGHEST, preferred_element_type=jnp.float32
    )
    local_row = chosen_pair - my_index * row_count
    is_mine = (local_row >= 0) & (local_row < row_count)
    before = lax.broadcasted_iota(jnp.int32, (capacity, capacity), 0)
    after = lax.broadcasted_iota(jnp.int32, (capacity, capacity), 1)
    slot_rank = jnp.dot(
        is_mine.astype(jnp.float32).astype(jnp.bfloat16),
        (before < after).astype(jnp.float32).astype(jnp.bfloat16),
        preferred_element_type=jnp.float32,
    ).astype(jnp.int32)
    row_ids = lax.broadcasted_iota(jnp.int32, (experts, row_count), 1)
    shifted = (local_row + 1).astype(jnp.float32)
    for m in range(most):
        match = is_mine & (slot_rank == m)
        target = jnp.sum(jnp.where(match, shifted, 0.0), axis=1, keepdims=True)
        gate = jnp.sum(jnp.where(match, gates_pair, 0.0), axis=1, keepdims=True)
        hit = target.astype(jnp.int32) - 1 == row_ids
        pick[:, m, :] = hit.astype(jnp.float32)
        gain_ref[:, m, :] = jnp.where(hit, gate, 0.0)


def project_kernel(
    replicas,
    count,
    x_hbm,
    w_hbm,
    residual_ref,
    norm_ref,
    chosen_ref,
    gates_ref,
    place_ref,
    state_ref,
    picked_ref,
    combine_ref,
    x_ref,
    w_ref,
    held,
    term,
    pick,
    load_sem,
    send_sem,
    recv_sem,
):
    dp = lax.axis_index("dp")
    rank = lax.axis_index("tensor")
    odd = rank % 2
    half = rank // 2
    here = (1 - odd) * half + odd * (count - 1 - half)
    right = ring_rank((here + 1) % count, count)
    left = ring_rank((here + count - 1) % count, count)
    rows = state_ref.shape[0]
    width = state_ref.shape[1] // LANES
    order = [lane for k in range(LANES // 2) for lane in (k, LANES // 2 + k)]

    def columns(lane):
        return slice(lane * width, (lane + 1) * width)

    loads = {
        lane: pltpu.make_async_copy(
            w_hbm.at[:, columns(lane)], w_ref.at[:, columns(lane)], load_sem.at[lane]
        )
        for lane in order
    }
    x_load = pltpu.make_async_copy(x_hbm, x_ref, load_sem.at[LANES])
    loads[order[0]].start()
    x_load.start()
    for lane in order[1:]:
        loads[lane].start()

    def own_term(lane, block):
        start = pl.multiple_of(ring_rank(block, count) * rows, rows)
        return jnp.dot(
            x_ref[pl.ds(start, rows), :],
            w_ref[:, columns(lane)],
            preferred_element_type=jnp.float32,
        )

    def block_of(lane, slot):
        if lane < LANES // 2:
            return (here + 2 * count - 1 - slot) % count
        return (here + 1 + slot) % count

    def copy(lane, slot):
        return pltpu.make_async_remote_copy(
            src_ref=held.at[lane, slot],
            dst_ref=held.at[lane, slot + 1],
            send_sem=send_sem.at[lane, slot],
            recv_sem=recv_sem.at[lane, slot + 1],
            device_id=(dp, right if lane < LANES // 2 else left),
            device_id_type=MESH,
        )

    def arrival(lane, slot):
        return pltpu.make_async_remote_copy(
            src_ref=held.at[lane, slot],
            dst_ref=held.at[lane, slot],
            send_sem=send_sem.at[lane, slot],
            recv_sem=recv_sem.at[lane, slot],
            device_id=(dp, right if lane < LANES // 2 else left),
            device_id_type=MESH,
        )

    barrier = pltpu.get_barrier_semaphore()
    for neighbour in (left, right):
        pl.semaphore_signal(barrier, inc=1, device_id=(dp, neighbour), device_id_type=MESH)
    x_load.wait()
    for n, lane in enumerate(order):
        loads[lane].wait()
        held[lane, 0] = own_term(lane, block_of(lane, 0)).astype(held.dtype)
        if n == 0:
            pl.semaphore_wait(barrier, 2)
        copy(lane, 0).start()

    routing(
        place_ref[...],
        chosen_ref[...],
        gates_ref[...],
        dp * count + rank,
        rows,
        pick,
        combine_ref,
    )

    def step(slot, carry):
        for lane in order:
            term[lane] = own_term(lane, block_of(lane, slot))
        for lane in order:
            arrival(lane, slot).wait_recv()
            held[lane, slot] = (held[lane, slot].astype(jnp.float32) + term[lane]).astype(held.dtype)
            copy(lane, slot).start()
        return carry

    lax.fori_loop(1, count - 1, step, 0)
    last = count - 1
    for lane in order:
        term[lane] = own_term(lane, block_of(lane, last)) + residual_ref[:, columns(lane)].astype(
            jnp.float32
        )
    total = jnp.zeros((rows, 1), jnp.float32)
    for lane in order:
        arrival(lane, last).wait_recv()
        state = held[lane, last].astype(jnp.float32) + term[lane]
        state_ref[:, columns(lane)] = state
        total = total + jnp.sum(state * state, axis=1, keepdims=True)
    scale = lax.rsqrt(total / (LANES * width) + 1.0)
    selector = pick[...].reshape(picked_ref.shape[0], rows).astype(jnp.bfloat16)
    for lane in order:
        normed = (state_ref[:, columns(lane)] * scale * norm_ref[:, columns(lane)]).astype(
            jnp.bfloat16
        )
        picked_ref[:, columns(lane)] = jnp.dot(
            selector, normed, preferred_element_type=jnp.float32
        ).astype(picked_ref.dtype)

    def drain(slot, carry):
        for lane in order:
            copy(lane, slot).wait_send()
        return carry

    lax.fori_loop(0, count - 1, drain, 0)


def project(x, w, residual, norm_gain, chosen, gates, place, replicas, count):
    rows, columns = residual.shape
    width = columns // LANES
    experts, capacity = chosen.shape
    most = 2 * capacity // (replicas * count)
    whole = pl.BlockSpec(memory_space=pltpu.VMEM)
    outside = pl.BlockSpec(memory_space=pl.ANY)
    return pl.pallas_call(
        functools.partial(project_kernel, replicas, count),
        out_shape=(
            jax.ShapeDtypeStruct((rows, columns), jnp.float32),
            jax.ShapeDtypeStruct((experts * most, columns), jnp.bfloat16),
            jax.ShapeDtypeStruct((experts, most, rows), jnp.float32),
        ),
        in_specs=[outside, outside] + [whole] * 5,
        out_specs=(whole, whole, whole),
        scratch_shapes=[
            pltpu.VMEM(x.shape, x.dtype),
            pltpu.VMEM(w.shape, w.dtype),
            pltpu.VMEM((LANES, count, rows, width), jnp.bfloat16),
            pltpu.VMEM((LANES, rows, width), jnp.float32),
            pltpu.VMEM((experts, most, rows), jnp.float32),
            pltpu.SemaphoreType.DMA((LANES + 1,)),
            pltpu.SemaphoreType.DMA((LANES, count)),
            pltpu.SemaphoreType.DMA((LANES, count)),
        ],
        compiler_params=pltpu.CompilerParams(
            collective_id=0, has_side_effects=True, vmem_limit_bytes=60 * 1024 * 1024
        ),
    )(x, w, residual, norm_gain[None, :], chosen, gates, place[None, :])


class Place:
    def __init__(self, replicas, count):
        self.dp = lax.axis_index("dp")
        rank = lax.axis_index("tensor")
        self.odd = rank % 2
        self.per_row = count // 2
        self.pairs = replicas * self.per_row
        self.pair = self.dp * self.per_row + rank // 2
        self.partner = (self.dp, rank + 1 - 2 * self.odd)

    def device(self, pair):
        return (pair // self.per_row, 2 * (pair % self.per_row) + self.odd)

    def toggle(self, number):
        replicas = self.pairs // self.per_row
        other = (number % replicas) * self.per_row + number // replicas
        total = 0
        bit = 1
        while bit < self.pairs:
            total = total + ((self.pair // bit + other // bit) % 2) * bit
            bit *= 2
        return total

    def greet(self):
        barrier = pltpu.get_barrier_semaphore()

        def signal(k, carry):
            target = self.device((self.pair + k) % self.pairs)
            pl.semaphore_signal(barrier, inc=1, device_id=target, device_id_type=MESH)
            return carry

        lax.fori_loop(1, self.pairs, signal, 0)
        pl.semaphore_signal(barrier, inc=1, device_id=self.partner, device_id_type=MESH)
        pl.semaphore_wait(barrier, self.pairs)


def loop(start, stop, body):
    def step(k, carry):
        body(k)
        return carry

    lax.fori_loop(start, stop, step, 0)


def experts_kernel(
    replicas,
    count,
    group,
    x_ref,
    state_ref,
    combine_ref,
    gate_hbm,
    up_hbm,
    down_hbm,
    out_ref,
    gate_w,
    up_w,
    down_w,
    received,
    result,
    part,
    returned,
    weight_sem,
    send_sem,
    pass_sem,
    recv_sem,
    cross_sem,
    part_sem,
    home_sem,
    done_sem,
):
    at = Place(replicas, count)
    most, width = x_ref.shape[1:]
    rows = group * 2 * most
    groups = at.pairs // group

    def source(k):
        return at.toggle(k)

    def outward(k):
        target = at.toggle(k)
        return pltpu.make_async_remote_copy(
            src_ref=x_ref.at[target],
            dst_ref=received.at[k, at.odd],
            send_sem=send_sem.at[k],
            recv_sem=recv_sem.at[k, at.odd],
            device_id=at.device(target),
            device_id_type=MESH,
        )

    def sideways(k, side):
        return pltpu.make_async_remote_copy(
            src_ref=received.at[k, side],
            dst_ref=received.at[k, side],
            send_sem=pass_sem.at[k],
            recv_sem=recv_sem.at[k, side],
            device_id=at.partner,
            device_id_type=MESH,
        )

    def across(k):
        return pltpu.make_async_remote_copy(
            src_ref=result.at[k, 1 - at.odd],
            dst_ref=part.at[k],
            send_sem=cross_sem.at[k],
            recv_sem=part_sem.at[k],
            device_id=at.partner,
            device_id_type=MESH,
        )

    def home(k):
        return pltpu.make_async_remote_copy(
            src_ref=part.at[k],
            dst_ref=returned.at[at.pair],
            send_sem=home_sem.at[k],
            recv_sem=done_sem.at[at.pair],
            device_id=at.device(source(k)),
            device_id_type=MESH,
        )

    def forward(k):
        sideways(k, at.odd).wait_recv()
        sideways(k, at.odd).start()

    def add(k):
        across(k).wait_recv()
        part[k] = (
            part[k].astype(jnp.float32) + result[k, at.odd].astype(jnp.float32)
        ).astype(part.dtype)

    def add_and_send(k):
        add(k)
        home(k).start()

    loads = [
        pltpu.make_async_copy(hbm.at[0], vmem, weight_sem.at[n])
        for n, (hbm, vmem) in enumerate(((gate_hbm, gate_w), (up_hbm, up_w), (down_hbm, down_w)))
    ]
    for load in loads:
        load.start()
    own = pltpu.make_async_remote_copy(
        src_ref=x_ref.at[at.pair],
        dst_ref=received.at[0, at.odd],
        send_sem=pass_sem.at[0],
        recv_sem=recv_sem.at[0, at.odd],
        device_id=at.partner,
        device_id_type=MESH,
    )
    at.greet()

    def members(g):
        return max(g * group, 1), (g + 1) * group

    for g in SEND_ORDER:
        loop(*members(g), lambda k: outward(k).start())
    own.start()
    received[0, at.odd] = x_ref[at.pair]
    for g in FORWARD_ORDER[:EARLY]:
        loop(*members(g), forward)
    for load in loads:
        load.wait()
    contract = (((1,), (1,)), ((), ()))
    late = FORWARD_ORDER[EARLY:]

    def code_of(numbers):
        return sum(number * groups**n for n, number in enumerate(numbers))

    def step(i, carry):
        compute_code, forward_code, before = carry
        first = (compute_code % groups) * group
        start = (forward_code % groups) * group

        def forward_piece(piece):
            @pl.when(i < len(late))
            def _():
                cut = [start + n * group // PIECES for n in (piece, piece + 1)]
                loop(jnp.maximum(cut[0], 1), cut[1], forward)

        loop(first, first + group, lambda k: sideways(k, 1 - at.odd).wait_recv())
        x = received[pl.ds(first, group)].reshape(rows, width)
        gate_part = lax.dot_general(x, gate_w[...], contract, preferred_element_type=jnp.float32)
        forward_piece(0)
        up_part = lax.dot_general(x, up_w[...], contract, preferred_element_type=jnp.float32)
        hidden = (gate_part / (1.0 + jnp.exp(-gate_part)) * up_part).astype(result.dtype)

        @pl.when(i > 0)
        def _():
            loop(jnp.maximum(before, 1), before + group, add_and_send)

        forward_piece(1)
        for piece in range(2):
            columns = slice(piece * (width // 2), (piece + 1) * (width // 2))
            y = jnp.dot(hidden, down_w[:, columns], preferred_element_type=jnp.float32)
            result[pl.ds(first, group), :, :, columns] = y.astype(result.dtype).reshape(
                group, 2, most, width // 2
            )
            forward_piece(2 + piece)
        loop(first, first + group, lambda k: across(k).start())
        return compute_code // groups, forward_code // groups, first

    lax.fori_loop(0, groups, step, (code_of(COMPUTE_ORDER), code_of(late), 0))
    loop(*members(COMPUTE_ORDER[-1]), add_and_send)
    add(0)
    returned[at.pair] = part[0]

    def settle(k):
        pair = source(k)
        pltpu.make_async_remote_copy(
            src_ref=part.at[k],
            dst_ref=returned.at[pair],
            send_sem=home_sem.at[k],
            recv_sem=done_sem.at[pair],
            device_id=at.partner,
            device_id_type=MESH,
        ).wait_recv()

    loop(1, at.pairs, settle)
    combine = combine_ref[...].reshape(at.pairs * most, state_ref.shape[0])
    coarse = combine.astype(jnp.bfloat16)
    fine = (combine - coarse.astype(jnp.float32)).astype(jnp.bfloat16)
    over_slots = (((0,), (0,)), ((), ()))
    for piece in range(PIECES):
        columns = slice(piece * (width // PIECES), (piece + 1) * (width // PIECES))
        slots = returned[:, :, columns].reshape(at.pairs * most, width // PIECES)
        moe = lax.dot_general(
            coarse, slots, over_slots, preferred_element_type=jnp.float32
        ) + lax.dot_general(fine, slots, over_slots, preferred_element_type=jnp.float32)
        out_ref[:, columns] = (state_ref[:, columns] + moe).astype(out_ref.dtype)
    own.wait_send()
    across(0).wait_send()

    def drain(k):
        outward(k).wait_send()
        sideways(k, at.odd).wait_send()
        across(k).wait_send()
        home(k).wait_send()

    loop(1, at.pairs, drain)


def experts_layer(x, state, combine, w_gate, w_up, w_down, replicas, count):
    pairs, most, width = x.shape
    group = pairs // len(COMPUTE_ORDER)
    hidden_units = w_gate.shape[1]
    weight = pltpu.VMEM((hidden_units, width), w_gate.dtype)
    slots = pltpu.VMEM((pairs, most, width), x.dtype)
    sides = pltpu.VMEM((pairs, 2, most, width), x.dtype)
    whole = pl.BlockSpec(memory_space=pltpu.VMEM)
    return pl.pallas_call(
        functools.partial(experts_kernel, replicas, count, group),
        out_shape=jax.ShapeDtypeStruct(state.shape, x.dtype),
        in_specs=[whole] * 3 + [pl.BlockSpec(memory_space=pl.ANY)] * 3,
        out_specs=whole,
        scratch_shapes=[
            weight,
            weight,
            weight,
            sides,
            sides,
            slots,
            slots,
            pltpu.SemaphoreType.DMA((3,)),
            pltpu.SemaphoreType.DMA((pairs,)),
            pltpu.SemaphoreType.DMA((pairs,)),
            pltpu.SemaphoreType.DMA((pairs, 2)),
            pltpu.SemaphoreType.DMA((pairs,)),
            pltpu.SemaphoreType.DMA((pairs,)),
            pltpu.SemaphoreType.DMA((pairs,)),
            pltpu.SemaphoreType.DMA((pairs,)),
        ],
        compiler_params=pltpu.CompilerParams(
            collective_id=1, has_side_effects=True, vmem_limit_bytes=60 * 1024 * 1024
        ),
    )(x, state, combine, w_gate, w_up, w_down)


def on_device(
    head_outputs, out_weight, residual, norm_gain, chosen, gates, place, w_gate, w_up, w_down
):
    count = lax.axis_size("tensor")
    replicas = lax.axis_size("dp")
    state, picked, combine = project(
        head_outputs, out_weight, residual, norm_gain, chosen, gates, place, replicas, count
    )
    experts, most = combine.shape[:2]
    picked = picked.reshape(experts, most, residual.shape[1])
    return experts_layer(picked, state, combine, w_gate, w_up, w_down, replicas, count)


def solution(mesh):
    return jax.shard_map(
        on_device,
        mesh=mesh,
        in_specs=(
            P("dp", "tensor"),
            P("tensor", None),
            P(("dp", "tensor"), None),
            P(),
            P(),
            P(),
            P(),
            P(("dp", "tensor"), None, None),
            P(("dp", "tensor"), None, None),
            P(("dp", "tensor"), None, None),
        ),
        out_specs=P(("dp", "tensor"), None),
        check_vma=False,
    )
```

```python
import functools

import jax
import jax.numpy as jnp
from jax import lax
from jax.experimental import pallas as pl
from jax.experimental.pallas import tpu as pltpu
from jax.sharding import PartitionSpec as P

MESH = pl.DeviceIdType.MESH
LANES = 4
PIECES = 4
GROUPS = 4
AHEAD = 2
SEND_ORDER = (1, 2, 3, 0)
HOME_ORDER = (2, 3, 1, 0)
ISSUE = ((2, (2,)), (3, (3, 1, 0)))


def ring_rank(position, count):
    upper = position // (count // 2)
    return (1 - upper) * 2 * position + upper * (2 * (count - 1 - position) + 1)


def routing(place, chosen, gates, my_index, row_count, pick, gain_ref):
    experts, capacity = chosen.shape
    most = pick.shape[1]
    pair_ids = lax.broadcasted_iota(jnp.int32, (experts, experts), 0)
    pair_map = (place == pair_ids).astype(jnp.float32)
    chosen_pair = jnp.dot(
        pair_map,
        chosen.astype(jnp.float32),
        precision=lax.Precision.HIGHEST,
        preferred_element_type=jnp.float32,
    ).astype(jnp.int32)
    gates_pair = jnp.dot(
        pair_map, gates, precision=lax.Precision.HIGHEST, preferred_element_type=jnp.float32
    )
    local_row = chosen_pair - my_index * row_count
    is_mine = (local_row >= 0) & (local_row < row_count)
    before = lax.broadcasted_iota(jnp.int32, (capacity, capacity), 0)
    after = lax.broadcasted_iota(jnp.int32, (capacity, capacity), 1)
    slot_rank = jnp.dot(
        is_mine.astype(jnp.float32).astype(jnp.bfloat16),
        (before < after).astype(jnp.float32).astype(jnp.bfloat16),
        preferred_element_type=jnp.float32,
    ).astype(jnp.int32)
    row_ids = lax.broadcasted_iota(jnp.int32, (experts, row_count), 1)
    shifted = (local_row + 1).astype(jnp.float32)
    for m in range(most):
        match = is_mine & (slot_rank == m)
        target = jnp.sum(jnp.where(match, shifted, 0.0), axis=1, keepdims=True)
        gate = jnp.sum(jnp.where(match, gates_pair, 0.0), axis=1, keepdims=True)
        hit = target.astype(jnp.int32) - 1 == row_ids
        pick[:, m, :] = hit.astype(jnp.float32)
        gain_ref[:, m, :] = jnp.where(hit, gate, 0.0)


def project_kernel(
    replicas,
    count,
    x_hbm,
    w_hbm,
    residual_ref,
    norm_ref,
    chosen_ref,
    gates_ref,
    place_ref,
    state_ref,
    picked_ref,
    combine_ref,
    x_ref,
    w_ref,
    held,
    term,
    pick,
    load_sem,
    send_sem,
    recv_sem,
):
    dp = lax.axis_index("dp")
    rank = lax.axis_index("tensor")
    odd = rank % 2
    half = rank // 2
    here = (1 - odd) * half + odd * (count - 1 - half)
    right = ring_rank((here + 1) % count, count)
    left = ring_rank((here + count - 1) % count, count)
    rows = state_ref.shape[0]
    width = state_ref.shape[1] // LANES
    order = [lane for k in range(LANES // 2) for lane in (k, LANES // 2 + k)]

    def columns(lane):
        return slice(lane * width, (lane + 1) * width)

    loads = {
        lane: pltpu.make_async_copy(
            w_hbm.at[:, columns(lane)], w_ref.at[:, columns(lane)], load_sem.at[lane]
        )
        for lane in order
    }
    x_load = pltpu.make_async_copy(x_hbm, x_ref, load_sem.at[LANES])
    loads[order[0]].start()
    x_load.start()
    for lane in order[1:]:
        loads[lane].start()

    def own_term(lane, block):
        start = pl.multiple_of(ring_rank(block, count) * rows, rows)
        return jnp.dot(
            x_ref[pl.ds(start, rows), :],
            w_ref[:, columns(lane)],
            preferred_element_type=jnp.float32,
        )

    def block_of(lane, slot):
        if lane < LANES // 2:
            return (here + 2 * count - 1 - slot) % count
        return (here + 1 + slot) % count

    def copy(lane, slot):
        return pltpu.make_async_remote_copy(
            src_ref=held.at[lane, slot],
            dst_ref=held.at[lane, slot + 1],
            send_sem=send_sem.at[lane, slot],
            recv_sem=recv_sem.at[lane, slot + 1],
            device_id=(dp, right if lane < LANES // 2 else left),
            device_id_type=MESH,
        )

    def arrival(lane, slot):
        return pltpu.make_async_remote_copy(
            src_ref=held.at[lane, slot],
            dst_ref=held.at[lane, slot],
            send_sem=send_sem.at[lane, slot],
            recv_sem=recv_sem.at[lane, slot],
            device_id=(dp, right if lane < LANES // 2 else left),
            device_id_type=MESH,
        )

    barrier = pltpu.get_barrier_semaphore()
    for neighbour in (left, right):
        pl.semaphore_signal(barrier, inc=1, device_id=(dp, neighbour), device_id_type=MESH)
    x_load.wait()
    for n, lane in enumerate(order):
        loads[lane].wait()
        held[lane, 0] = own_term(lane, block_of(lane, 0)).astype(held.dtype)
        if n == 0:
            pl.semaphore_wait(barrier, 2)
        copy(lane, 0).start()

    routing(
        place_ref[...],
        chosen_ref[...],
        gates_ref[...],
        dp * count + rank,
        rows,
        pick,
        combine_ref,
    )

    def step(slot, carry):
        for lane in order:
            term[lane] = own_term(lane, block_of(lane, slot))
        for lane in order:
            arrival(lane, slot).wait_recv()
            held[lane, slot] = (held[lane, slot].astype(jnp.float32) + term[lane]).astype(held.dtype)
            copy(lane, slot).start()
        return carry

    lax.fori_loop(1, count - 1, step, 0)
    last = count - 1
    for lane in order:
        term[lane] = own_term(lane, block_of(lane, last)) + residual_ref[:, columns(lane)].astype(
            jnp.float32
        )
    total = jnp.zeros((rows, 1), jnp.float32)
    for lane in order:
        arrival(lane, last).wait_recv()
        state = held[lane, last].astype(jnp.float32) + term[lane]
        state_ref[:, columns(lane)] = state
        total = total + jnp.sum(state * state, axis=1, keepdims=True)
    scale = lax.rsqrt(total / (LANES * width) + 1.0)
    selector = pick[...].reshape(picked_ref.shape[0], rows).astype(jnp.bfloat16)
    for lane in order:
        normed = (state_ref[:, columns(lane)] * scale * norm_ref[:, columns(lane)]).astype(
            jnp.bfloat16
        )
        picked_ref[:, columns(lane)] = jnp.dot(
            selector, normed, preferred_element_type=jnp.float32
        ).astype(picked_ref.dtype)

    def drain(slot, carry):
        for lane in order:
            copy(lane, slot).wait_send()
        return carry

    lax.fori_loop(0, count - 1, drain, 0)


def project(x, w, residual, norm_gain, chosen, gates, place, replicas, count):
    rows, columns = residual.shape
    width = columns // LANES
    experts, capacity = chosen.shape
    most = 2 * capacity // (replicas * count)
    whole = pl.BlockSpec(memory_space=pltpu.VMEM)
    outside = pl.BlockSpec(memory_space=pl.ANY)
    return pl.pallas_call(
        functools.partial(project_kernel, replicas, count),
        out_shape=(
            jax.ShapeDtypeStruct((rows, columns), jnp.float32),
            jax.ShapeDtypeStruct((experts * most, columns), jnp.bfloat16),
            jax.ShapeDtypeStruct((experts, most, rows), jnp.float32),
        ),
        in_specs=[outside, outside] + [whole] * 5,
        out_specs=(whole, whole, whole),
        scratch_shapes=[
            pltpu.VMEM(x.shape, x.dtype),
            pltpu.VMEM(w.shape, w.dtype),
            pltpu.VMEM((LANES, count, rows, width), jnp.bfloat16),
            pltpu.VMEM((LANES, rows, width), jnp.float32),
            pltpu.VMEM((experts, most, rows), jnp.float32),
            pltpu.SemaphoreType.DMA((LANES + 1,)),
            pltpu.SemaphoreType.DMA((LANES, count)),
            pltpu.SemaphoreType.DMA((LANES, count)),
        ],
        compiler_params=pltpu.CompilerParams(
            collective_id=0, has_side_effects=True, vmem_limit_bytes=44 * 1024 * 1024
        ),
    )(x, w, residual, norm_gain[None, :], chosen, gates, place[None, :])


def flip(value, bit):
    return value + bit - 2 * bit * ((value // bit) % 2)


def toggled(value, mask):
    bit = 1
    while bit <= mask:
        if mask & bit:
            value = flip(value, bit)
        bit *= 2
    return value


def exchange_kernel(
    replicas,
    x_hbm,
    w_hbm,
    residual_ref,
    norm_ref,
    chosen_ref,
    gates_ref,
    place_ref,
    state_ref,
    picked_ref,
    combine_ref,
    lhs,
    rhs,
    side_out,
    side_in,
    far_out,
    far_in,
    pick,
    load_sem,
    rows_send,
    rows_recv,
    cols_send,
    cols_recv,
    relay_sem,
    side_send,
    side_recv,
    far_send,
    far_recv,
):
    dp = lax.axis_index("dp")
    rank = lax.axis_index("tensor")
    near, side, far = flip(rank, 2), flip(rank, 1), flip(rank, 4)
    rows, total = state_ref.shape
    depth = x_hbm.shape[1]
    share = total // replicas
    width = share // PIECES
    bits = [1 << n for n in range(replicas.bit_length() - 1)]
    blocks = [(n, 1 - n // 2, n % 2) for n in range(4)]

    def place_of(owner, other_side, other_far):
        mask = other_side + 4 * other_far
        return pl.multiple_of(toggled(owner, mask) * rows, rows)

    def cols(origin, piece):
        return pl.ds(pl.multiple_of(origin * share + piece * width, width), width)

    def rows_copy(n, other_side, other_far):
        return pltpu.make_async_remote_copy(
            src_ref=x_hbm.at[pl.ds(place_of(near, other_side, other_far), rows), :],
            dst_ref=lhs.at[n * rows : (n + 1) * rows, depth:],
            send_sem=rows_send.at[n],
            recv_sem=rows_recv.at[n],
            device_id=(dp, near),
            device_id_type=MESH,
        )

    def cols_copy(piece):
        return pltpu.make_async_remote_copy(
            src_ref=w_hbm.at[:, cols(dp, piece)],
            dst_ref=rhs.at[depth:, cols(dp, piece)],
            send_sem=cols_send.at[piece],
            recv_sem=cols_recv.at[piece, 0],
            device_id=(dp, near),
            device_id_type=MESH,
        )

    def relay(piece, origin, bit):
        window = rhs.at[depth:, cols(toggled(dp, origin), piece)]
        return pltpu.make_async_remote_copy(
            src_ref=window,
            dst_ref=window,
            send_sem=relay_sem.at[piece, origin, bits.index(bit)],
            recv_sem=cols_recv.at[piece, origin ^ bit],
            device_id=(flip(dp, bit), rank),
            device_id_type=MESH,
        )

    def cols_arrival(piece, origin):
        window = rhs.at[depth:, cols(toggled(dp, origin), piece)]
        return pltpu.make_async_remote_copy(
            src_ref=window,
            dst_ref=window,
            send_sem=cols_send.at[piece],
            recv_sem=cols_recv.at[piece, origin],
            device_id=(dp, near),
            device_id_type=MESH,
        )

    def onward(origin):
        return [bit for bit in bits if origin % (2 * bit) == 0]

    def side_copy(piece, origin):
        n = piece * replicas + origin
        return pltpu.make_async_remote_copy(
            src_ref=side_out.at[n],
            dst_ref=side_in.at[n],
            send_sem=side_send.at[n],
            recv_sem=side_recv.at[n],
            device_id=(dp, side),
            device_id_type=MESH,
        )

    def far_copy(piece, origin):
        n = piece * replicas + origin
        return pltpu.make_async_remote_copy(
            src_ref=far_out.at[n],
            dst_ref=far_in.at[n],
            send_sem=far_send.at[n],
            recv_sem=far_recv.at[n],
            device_id=(dp, far),
            device_id_type=MESH,
        )

    w_load = pltpu.make_async_copy(w_hbm, rhs.at[:depth, :], load_sem.at[0])
    x_loads = [
        pltpu.make_async_copy(
            x_hbm.at[pl.ds(place_of(rank, other_side, other_far), rows), :],
            lhs.at[n * rows : (n + 1) * rows, :depth],
            load_sem.at[1 + n],
        )
        for n, other_side, other_far in blocks
    ]
    barrier = pltpu.get_barrier_semaphore()
    partners = [(dp, near), (dp, side), (dp, far)] + [(flip(dp, bit), rank) for bit in bits]
    for partner in partners:
        pl.semaphore_signal(barrier, inc=1, device_id=partner, device_id_type=MESH)
    w_load.start()
    for load in x_loads:
        load.start()
    pl.semaphore_wait(barrier, len(partners))
    for block in blocks[:2]:
        rows_copy(*block).start()
    cols_copy(0).start()
    for block in blocks[2:]:
        rows_copy(*block).start()
    for piece in range(1, PIECES):
        cols_copy(piece).start()
    routing(
        place_ref[...],
        chosen_ref[...],
        gates_ref[...],
        dp * lax.axis_size("tensor") + rank,
        rows,
        pick,
        combine_ref,
    )
    w_load.wait()
    for load in x_loads:
        load.wait()
    for block in blocks[:2]:
        rows_copy(*block).wait_recv()

    def begin(piece, origin):
        cols_arrival(piece, origin).wait_recv()
        for bit in onward(origin):
            relay(piece, origin, bit).start()
        here = cols(toggled(dp, origin), piece)
        side_out[piece * replicas + origin] = jnp.dot(
            lhs[: 2 * rows, :], rhs[:, here], preferred_element_type=jnp.float32
        ).astype(side_out.dtype)
        side_copy(piece, origin).start()

    def middle(piece, origin):
        n = piece * replicas + origin
        here = cols(toggled(dp, origin), piece)
        own = jnp.dot(lhs[2 * rows :, :], rhs[:, here], preferred_element_type=jnp.float32)
        side_copy(piece, origin).wait_recv()
        both = own + side_in[n].astype(jnp.float32)
        far_out[n] = both[rows:].astype(far_out.dtype)
        far_copy(piece, origin).start()
        state_ref[:, here] = both[:rows] + residual_ref[:, here].astype(jnp.float32)

    begin(0, 0)
    begin(0, 1)
    for block in blocks[2:]:
        rows_copy(*block).wait_recv()

    def step(piece, carry):
        for origin in range(replicas):
            if origin < 2:

                @pl.when(piece > 0)
                def _():
                    begin(piece, origin)
                    middle(piece - 1, origin + replicas - 2)

            else:
                begin(piece, origin)
                middle(piece, origin - 2)
        return carry

    lax.fori_loop(0, PIECES, step, 0)
    middle(PIECES - 1, replicas - 2)
    middle(PIECES - 1, replicas - 1)

    def finish(piece, squares):
        for origin in range(replicas):
            here = cols(toggled(dp, origin), piece)
            far_copy(piece, origin).wait_recv()
            state = state_ref[:, here] + far_in[piece * replicas + origin].astype(jnp.float32)
            state_ref[:, here] = state
            squares = squares + jnp.sum(state * state, axis=1, keepdims=True)
        return squares

    squares = lax.fori_loop(0, PIECES, finish, jnp.zeros((rows, 1), jnp.float32))
    scale = lax.rsqrt(squares / total + 1.0)
    selector = pick[...].reshape(picked_ref.shape[0], rows).astype(jnp.bfloat16)
    for lane in range(LANES):
        here = slice(lane * (total // LANES), (lane + 1) * (total // LANES))
        normed = (state_ref[:, here] * scale * norm_ref[:, here]).astype(jnp.bfloat16)
        picked_ref[:, here] = jnp.dot(
            selector, normed, preferred_element_type=jnp.float32
        ).astype(picked_ref.dtype)
    for block in blocks:
        rows_copy(*block).wait_send()

    def drain(piece, carry):
        cols_copy(piece).wait_send()
        for origin in range(replicas):
            for bit in onward(origin):
                relay(piece, origin, bit).wait_send()
            side_copy(piece, origin).wait_send()
            far_copy(piece, origin).wait_send()
        return carry

    lax.fori_loop(0, PIECES, drain, 0)


def exchange(x, w, residual, norm_gain, chosen, gates, place, replicas, count):
    rows, columns = residual.shape
    depth = x.shape[1]
    width = columns // replicas // PIECES
    number = replicas * PIECES
    experts, capacity = chosen.shape
    most = 2 * capacity // (replicas * count)
    whole = pl.BlockSpec(memory_space=pltpu.VMEM)
    outside = pl.BlockSpec(memory_space=pl.ANY)
    dma = pltpu.SemaphoreType.DMA
    return pl.pallas_call(
        functools.partial(exchange_kernel, replicas),
        out_shape=(
            jax.ShapeDtypeStruct((rows, columns), jnp.float32),
            jax.ShapeDtypeStruct((experts * most, columns), jnp.bfloat16),
            jax.ShapeDtypeStruct((experts, most, rows), jnp.float32),
        ),
        in_specs=[outside, outside] + [whole] * 5,
        out_specs=(whole, whole, whole),
        scratch_shapes=[
            pltpu.VMEM((4 * rows, 2 * depth), x.dtype),
            pltpu.VMEM((2 * depth, columns), w.dtype),
            pltpu.VMEM((number, 2 * rows, width), jnp.bfloat16),
            pltpu.VMEM((number, 2 * rows, width), jnp.bfloat16),
            pltpu.VMEM((number, rows, width), jnp.bfloat16),
            pltpu.VMEM((number, rows, width), jnp.bfloat16),
            pltpu.VMEM((experts, most, rows), jnp.float32),
            dma((5,)),
            dma((4,)),
            dma((4,)),
            dma((PIECES,)),
            dma((PIECES, replicas)),
            dma((PIECES, replicas, replicas.bit_length() - 1)),
            dma((number,)),
            dma((number,)),
            dma((number,)),
            dma((number,)),
        ],
        compiler_params=pltpu.CompilerParams(
            collective_id=2, has_side_effects=True, vmem_limit_bytes=44 * 1024 * 1024
        ),
    )(x, w, residual, norm_gain[None, :], chosen, gates, place[None, :])


class Place:
    def __init__(self, replicas, count):
        self.dp = lax.axis_index("dp")
        rank = lax.axis_index("tensor")
        self.odd = rank % 2
        self.per_row = count // 2
        self.pairs = replicas * self.per_row
        self.pair = self.dp * self.per_row + rank // 2
        self.partner = (self.dp, rank + 1 - 2 * self.odd)

    def device(self, pair):
        return (pair // self.per_row, 2 * (pair % self.per_row) + self.odd)

    def toggle(self, number):
        replicas = self.pairs // self.per_row
        near = number // replicas, number % replicas
        beyond = number - self.pairs // 2
        steps = self.per_row // 2
        far = steps + beyond % steps, beyond // steps
        is_far = number // (self.pairs // 2)
        row, column = (is_far * b + (1 - is_far) * a for a, b in zip(near, far))
        other = column * self.per_row + row
        total = 0
        bit = 1
        while bit < self.pairs:
            total = total + ((self.pair // bit + other // bit) % 2) * bit
            bit *= 2
        return total

    def greet(self):
        barrier = pltpu.get_barrier_semaphore()

        def signal(k, carry):
            target = self.device((self.pair + k) % self.pairs)
            pl.semaphore_signal(barrier, inc=1, device_id=target, device_id_type=MESH)
            return carry

        lax.fori_loop(1, self.pairs, signal, 0)
        pl.semaphore_signal(barrier, inc=1, device_id=self.partner, device_id_type=MESH)
        pl.semaphore_wait(barrier, self.pairs)


def loop(start, stop, body):
    def step(k, carry):
        body(k)
        return carry

    lax.fori_loop(start, stop, step, 0)


def experts_kernel(
    replicas,
    count,
    group,
    x_ref,
    state_ref,
    combine_ref,
    gate_hbm,
    up_hbm,
    down_hbm,
    out_ref,
    gate_w,
    up_w,
    down_w,
    received,
    result,
    part,
    returned,
    weight_sem,
    send_sem,
    pass_sem,
    recv_sem,
    cross_sem,
    part_sem,
    home_sem,
    done_sem,
):
    at = Place(replicas, count)
    most, width = x_ref.shape[1:]
    rows = group * 2 * most
    groups = at.pairs // group

    def source(k):
        return at.toggle(k)

    def outward(k):
        target = at.toggle(k)
        return pltpu.make_async_remote_copy(
            src_ref=x_ref.at[target],
            dst_ref=received.at[k, at.odd],
            send_sem=send_sem.at[k],
            recv_sem=recv_sem.at[k, at.odd],
            device_id=at.device(target),
            device_id_type=MESH,
        )

    def sideways(k, side):
        return pltpu.make_async_remote_copy(
            src_ref=received.at[k, side],
            dst_ref=received.at[k, side],
            send_sem=pass_sem.at[k],
            recv_sem=recv_sem.at[k, side],
            device_id=at.partner,
            device_id_type=MESH,
        )

    def across(k):
        return pltpu.make_async_remote_copy(
            src_ref=result.at[k, 1 - at.odd],
            dst_ref=part.at[k],
            send_sem=cross_sem.at[k],
            recv_sem=part_sem.at[k],
            device_id=at.partner,
            device_id_type=MESH,
        )

    def home(k):
        return pltpu.make_async_remote_copy(
            src_ref=part.at[k],
            dst_ref=returned.at[at.pair],
            send_sem=home_sem.at[k],
            recv_sem=done_sem.at[at.pair],
            device_id=at.device(source(k)),
            device_id_type=MESH,
        )

    def forward(k):
        sideways(k, at.odd).wait_recv()
        sideways(k, at.odd).start()

    def add(k):
        across(k).wait_recv()
        part[k] = (
            part[k].astype(jnp.float32) + result[k, at.odd].astype(jnp.float32)
        ).astype(part.dtype)

    def add_and_send(k):
        add(k)
        home(k).start()

    loads = [
        pltpu.make_async_copy(hbm.at[0], vmem, weight_sem.at[n])
        for n, (hbm, vmem) in enumerate(((gate_hbm, gate_w), (up_hbm, up_w), (down_hbm, down_w)))
    ]
    for load in loads:
        load.start()
    own = pltpu.make_async_remote_copy(
        src_ref=x_ref.at[at.pair],
        dst_ref=received.at[0, at.odd],
        send_sem=pass_sem.at[0],
        recv_sem=recv_sem.at[0, at.odd],
        device_id=at.partner,
        device_id_type=MESH,
    )
    at.greet()

    def members(g):
        return max(g * group, 1), (g + 1) * group

    for g in SEND_ORDER:
        loop(*members(g), lambda k: outward(k).start())
    own.start()
    received[0, at.odd] = x_ref[at.pair]
    for g in range(AHEAD):
        loop(*members(g), forward)
    for load in loads:
        load.wait()
    contract = (((1,), (1,)), ((), ()))

    def step(g, carry):
        first = g * group
        start = first + AHEAD * group

        def forward_piece(piece):
            @pl.when(g + AHEAD < GROUPS)
            def _():
                cut = [start + n * group // PIECES for n in (piece, piece + 1)]
                loop(cut[0], cut[1], forward)

        loop(first, first + group, lambda k: sideways(k, 1 - at.odd).wait_recv())
        x = received[pl.ds(first, group)].reshape(rows, width)
        gate_part = lax.dot_general(x, gate_w[...], contract, preferred_element_type=jnp.float32)
        forward_piece(0)
        up_part = lax.dot_general(x, up_w[...], contract, preferred_element_type=jnp.float32)
        hidden = (gate_part / (1.0 + jnp.exp(-gate_part)) * up_part).astype(result.dtype)
        forward_piece(1)
        for piece in range(2):
            columns = slice(piece * (width // 2), (piece + 1) * (width // 2))
            y = jnp.dot(hidden, down_w[:, columns], preferred_element_type=jnp.float32)
            result[pl.ds(first, group), :, :, columns] = y.astype(result.dtype).reshape(
                group, 2, most, width // 2
            )
            forward_piece(2 + piece)

        for n, sets in ISSUE:
            @pl.when(g == n)
            def _():
                for h in sets:
                    crossing(h)

        return carry

    def crossing(g):
        loop(0, group, lambda k: across((g + 1) * group - 1 - k).start())

    def homeward(g):
        low, high = members(g)
        loop(0, high - low, lambda k: add_and_send(high - 1 - k))

    lax.fori_loop(0, GROUPS, step, 0)
    for g in HOME_ORDER:
        homeward(g)
    add(0)
    returned[at.pair] = part[0]

    def settle(k):
        pair = source(k)
        pltpu.make_async_remote_copy(
            src_ref=part.at[k],
            dst_ref=returned.at[pair],
            send_sem=home_sem.at[k],
            recv_sem=done_sem.at[pair],
            device_id=at.partner,
            device_id_type=MESH,
        ).wait_recv()

    loop(1, at.pairs, settle)
    combine = combine_ref[...].reshape(at.pairs * most, state_ref.shape[0])
    coarse = combine.astype(jnp.bfloat16)
    fine = (combine - coarse.astype(jnp.float32)).astype(jnp.bfloat16)
    over_slots = (((0,), (0,)), ((), ()))
    for piece in range(PIECES):
        columns = slice(piece * (width // PIECES), (piece + 1) * (width // PIECES))
        slots = returned[:, :, columns].reshape(at.pairs * most, width // PIECES)
        moe = lax.dot_general(
            coarse, slots, over_slots, preferred_element_type=jnp.float32
        ) + lax.dot_general(fine, slots, over_slots, preferred_element_type=jnp.float32)
        out_ref[:, columns] = (state_ref[:, columns] + moe).astype(out_ref.dtype)
    own.wait_send()
    across(0).wait_send()

    def drain(k):
        outward(k).wait_send()
        sideways(k, at.odd).wait_send()
        across(k).wait_send()
        home(k).wait_send()

    loop(1, at.pairs, drain)


def experts_layer(x, state, combine, w_gate, w_up, w_down, replicas, count):
    pairs, most, width = x.shape
    group = pairs // GROUPS
    hidden_units = w_gate.shape[1]
    weight = pltpu.VMEM((hidden_units, width), w_gate.dtype)
    slots = pltpu.VMEM((pairs, most, width), x.dtype)
    sides = pltpu.VMEM((pairs, 2, most, width), x.dtype)
    whole = pl.BlockSpec(memory_space=pltpu.VMEM)
    return pl.pallas_call(
        functools.partial(experts_kernel, replicas, count, group),
        out_shape=jax.ShapeDtypeStruct(state.shape, x.dtype),
        in_specs=[whole] * 3 + [pl.BlockSpec(memory_space=pl.ANY)] * 3,
        out_specs=whole,
        scratch_shapes=[
            weight,
            weight,
            weight,
            sides,
            sides,
            slots,
            slots,
            pltpu.SemaphoreType.DMA((3,)),
            pltpu.SemaphoreType.DMA((pairs,)),
            pltpu.SemaphoreType.DMA((pairs,)),
            pltpu.SemaphoreType.DMA((pairs, 2)),
            pltpu.SemaphoreType.DMA((pairs,)),
            pltpu.SemaphoreType.DMA((pairs,)),
            pltpu.SemaphoreType.DMA((pairs,)),
            pltpu.SemaphoreType.DMA((pairs,)),
        ],
        compiler_params=pltpu.CompilerParams(
            collective_id=1, has_side_effects=True, vmem_limit_bytes=44 * 1024 * 1024
        ),
    )(x, state, combine, w_gate, w_up, w_down)


def on_device(
    head_outputs, out_weight, residual, norm_gain, chosen, gates, place, w_gate, w_up, w_down
):
    count = lax.axis_size("tensor")
    replicas = lax.axis_size("dp")
    first = exchange if count == 8 and replicas >= 4 else project
    state, picked, combine = first(
        head_outputs, out_weight, residual, norm_gain, chosen, gates, place, replicas, count
    )
    experts, most = combine.shape[:2]
    picked = picked.reshape(experts, most, residual.shape[1])
    return experts_layer(picked, state, combine, w_gate, w_up, w_down, replicas, count)


def solution(mesh):
    return jax.shard_map(
        on_device,
        mesh=mesh,
        in_specs=(
            P("dp", "tensor"),
            P("tensor", None),
            P(("dp", "tensor"), None),
            P(),
            P(),
            P(),
            P(),
            P(("dp", "tensor"), None, None),
            P(("dp", "tensor"), None, None),
            P(("dp", "tensor"), None, None),
        ),
        out_specs=P(("dp", "tensor"), None),
        check_vma=False,
    )
```

```python
import functools

import jax
import jax.numpy as jnp
from jax import lax
from jax.experimental import pallas as pl
from jax.experimental.pallas import tpu as pltpu
from jax.sharding import PartitionSpec as P

MESH = pl.DeviceIdType.MESH
LANES = 4
PIECES = 4
GROUPS = 4
FIRST = 17
LIMIT = 58
AHEAD = 2
SEND_ORDER = (1, 2, 3, 0)
HOME_ORDER = (2, 3, 1, 0)
ISSUE = ((2, (2,)), (3, (3, 1, 0)))


def ring_rank(position, count):
    upper = position // (count // 2)
    return (1 - upper) * 2 * position + upper * (2 * (count - 1 - position) + 1)


def routing(place, chosen, gates, my_index, row_count, pick, gain_ref):
    experts, capacity = chosen.shape
    most = pick.shape[1]
    pair_ids = lax.broadcasted_iota(jnp.int32, (experts, experts), 0)
    pair_map = (place == pair_ids).astype(jnp.float32)
    chosen_pair = jnp.dot(
        pair_map,
        chosen.astype(jnp.float32),
        precision=lax.Precision.HIGHEST,
        preferred_element_type=jnp.float32,
    ).astype(jnp.int32)
    gates_pair = jnp.dot(
        pair_map, gates, precision=lax.Precision.HIGHEST, preferred_element_type=jnp.float32
    )
    local_row = chosen_pair - my_index * row_count
    is_mine = (local_row >= 0) & (local_row < row_count)
    before = lax.broadcasted_iota(jnp.int32, (capacity, capacity), 0)
    after = lax.broadcasted_iota(jnp.int32, (capacity, capacity), 1)
    slot_rank = jnp.dot(
        is_mine.astype(jnp.float32).astype(jnp.bfloat16),
        (before < after).astype(jnp.float32).astype(jnp.bfloat16),
        preferred_element_type=jnp.float32,
    ).astype(jnp.int32)
    row_ids = lax.broadcasted_iota(jnp.int32, (experts, row_count), 1)
    shifted = (local_row + 1).astype(jnp.float32)
    for m in range(most):
        match = is_mine & (slot_rank == m)
        target = jnp.sum(jnp.where(match, shifted, 0.0), axis=1, keepdims=True)
        gate = jnp.sum(jnp.where(match, gates_pair, 0.0), axis=1, keepdims=True)
        hit = target.astype(jnp.int32) - 1 == row_ids
        pick[:, m, :] = hit.astype(jnp.float32)
        gain_ref[:, m, :] = jnp.where(hit, gate, 0.0)


def project_kernel(
    replicas,
    count,
    x_hbm,
    w_hbm,
    residual_ref,
    norm_ref,
    chosen_ref,
    gates_ref,
    place_ref,
    state_ref,
    picked_ref,
    combine_ref,
    x_ref,
    w_ref,
    held,
    term,
    pick,
    load_sem,
    send_sem,
    recv_sem,
):
    dp = lax.axis_index("dp")
    rank = lax.axis_index("tensor")
    odd = rank % 2
    half = rank // 2
    here = (1 - odd) * half + odd * (count - 1 - half)
    right = ring_rank((here + 1) % count, count)
    left = ring_rank((here + count - 1) % count, count)
    rows = state_ref.shape[0]
    width = state_ref.shape[1] // LANES
    order = [lane for k in range(LANES // 2) for lane in (k, LANES // 2 + k)]

    def columns(lane):
        return slice(lane * width, (lane + 1) * width)

    loads = {
        lane: pltpu.make_async_copy(
            w_hbm.at[:, columns(lane)], w_ref.at[:, columns(lane)], load_sem.at[lane]
        )
        for lane in order
    }
    x_load = pltpu.make_async_copy(x_hbm, x_ref, load_sem.at[LANES])
    loads[order[0]].start()
    x_load.start()
    for lane in order[1:]:
        loads[lane].start()

    def own_term(lane, block):
        start = pl.multiple_of(ring_rank(block, count) * rows, rows)
        return jnp.dot(
            x_ref[pl.ds(start, rows), :],
            w_ref[:, columns(lane)],
            preferred_element_type=jnp.float32,
        )

    def block_of(lane, slot):
        if lane < LANES // 2:
            return (here + 2 * count - 1 - slot) % count
        return (here + 1 + slot) % count

    def copy(lane, slot):
        return pltpu.make_async_remote_copy(
            src_ref=held.at[lane, slot],
            dst_ref=held.at[lane, slot + 1],
            send_sem=send_sem.at[lane, slot],
            recv_sem=recv_sem.at[lane, slot + 1],
            device_id=(dp, right if lane < LANES // 2 else left),
            device_id_type=MESH,
        )

    def arrival(lane, slot):
        return pltpu.make_async_remote_copy(
            src_ref=held.at[lane, slot],
            dst_ref=held.at[lane, slot],
            send_sem=send_sem.at[lane, slot],
            recv_sem=recv_sem.at[lane, slot],
            device_id=(dp, right if lane < LANES // 2 else left),
            device_id_type=MESH,
        )

    barrier = pltpu.get_barrier_semaphore()
    for neighbour in (left, right):
        pl.semaphore_signal(barrier, inc=1, device_id=(dp, neighbour), device_id_type=MESH)
    x_load.wait()
    for n, lane in enumerate(order):
        loads[lane].wait()
        held[lane, 0] = own_term(lane, block_of(lane, 0)).astype(held.dtype)
        if n == 0:
            pl.semaphore_wait(barrier, 2)
        copy(lane, 0).start()

    routing(
        place_ref[...],
        chosen_ref[...],
        gates_ref[...],
        dp * count + rank,
        rows,
        pick,
        combine_ref,
    )

    def step(slot, carry):
        for lane in order:
            term[lane] = own_term(lane, block_of(lane, slot))
        for lane in order:
            arrival(lane, slot).wait_recv()
            held[lane, slot] = (held[lane, slot].astype(jnp.float32) + term[lane]).astype(held.dtype)
            copy(lane, slot).start()
        return carry

    lax.fori_loop(1, count - 1, step, 0)
    last = count - 1
    for lane in order:
        term[lane] = own_term(lane, block_of(lane, last)) + residual_ref[:, columns(lane)].astype(
            jnp.float32
        )
    total = jnp.zeros((rows, 1), jnp.float32)
    for lane in order:
        arrival(lane, last).wait_recv()
        state = held[lane, last].astype(jnp.float32) + term[lane]
        state_ref[:, columns(lane)] = state
        total = total + jnp.sum(state * state, axis=1, keepdims=True)
    scale = lax.rsqrt(total / (LANES * width) + 1.0)
    selector = pick[...].reshape(picked_ref.shape[0], rows).astype(jnp.bfloat16)
    for lane in order:
        normed = (state_ref[:, columns(lane)] * scale * norm_ref[:, columns(lane)]).astype(
            jnp.bfloat16
        )
        picked_ref[:, columns(lane)] = jnp.dot(
            selector, normed, preferred_element_type=jnp.float32
        ).astype(picked_ref.dtype)

    def drain(slot, carry):
        for lane in order:
            copy(lane, slot).wait_send()
        return carry

    lax.fori_loop(0, count - 1, drain, 0)


def project(x, w, residual, norm_gain, chosen, gates, place, replicas, count):
    rows, columns = residual.shape
    width = columns // LANES
    experts, capacity = chosen.shape
    most = 2 * capacity // (replicas * count)
    whole = pl.BlockSpec(memory_space=pltpu.VMEM)
    outside = pl.BlockSpec(memory_space=pl.ANY)
    return pl.pallas_call(
        functools.partial(project_kernel, replicas, count),
        out_shape=(
            jax.ShapeDtypeStruct((rows, columns), jnp.float32),
            jax.ShapeDtypeStruct((experts * most, columns), jnp.bfloat16),
            jax.ShapeDtypeStruct((experts, most, rows), jnp.float32),
        ),
        in_specs=[outside, outside] + [whole] * 5,
        out_specs=(whole, whole, whole),
        scratch_shapes=[
            pltpu.VMEM(x.shape, x.dtype),
            pltpu.VMEM(w.shape, w.dtype),
            pltpu.VMEM((LANES, count, rows, width), jnp.bfloat16),
            pltpu.VMEM((LANES, rows, width), jnp.float32),
            pltpu.VMEM((experts, most, rows), jnp.float32),
            pltpu.SemaphoreType.DMA((LANES + 1,)),
            pltpu.SemaphoreType.DMA((LANES, count)),
            pltpu.SemaphoreType.DMA((LANES, count)),
        ],
        compiler_params=pltpu.CompilerParams(
            collective_id=0, has_side_effects=True, vmem_limit_bytes=44 * 1024 * 1024
        ),
    )(x, w, residual, norm_gain[None, :], chosen, gates, place[None, :])


def flip(value, bit):
    return value + bit - 2 * bit * ((value // bit) % 2)


def toggled(value, mask):
    bit = 1
    while bit <= mask:
        if mask & bit:
            value = flip(value, bit)
        bit *= 2
    return value


def exchange_phase(
    replicas,
    greet,
    x_hbm,
    w_hbm,
    small,
    state_ref,
    picked_ref,
    combine_ref,
    residual_ref,
    norm_ref,
    chosen_ref,
    gates_ref,
    place_ref,
    lhs,
    rhs,
    side_out,
    side_in,
    far_out,
    far_in,
    pick,
    load_sem,
    rows_send,
    rows_recv,
    cols_send,
    cols_recv,
    relay_sem,
    side_send,
    side_recv,
    far_send,
    far_recv,
):
    dp = lax.axis_index("dp")
    rank = lax.axis_index("tensor")
    near, side, far = flip(rank, 2), flip(rank, 1), flip(rank, 4)
    rows, total = state_ref.shape
    depth = x_hbm.shape[1]
    share = total // replicas
    width = share // PIECES
    bits = [1 << n for n in range(replicas.bit_length() - 1)]
    blocks = [(n, 1 - n // 2, n % 2) for n in range(4)]

    def place_of(owner, other_side, other_far):
        mask = other_side + 4 * other_far
        return pl.multiple_of(toggled(owner, mask) * rows, rows)

    def cols(origin, piece):
        return pl.ds(pl.multiple_of(origin * share + piece * width, width), width)

    def rows_copy(n, other_side, other_far):
        return pltpu.make_async_remote_copy(
            src_ref=x_hbm.at[pl.ds(place_of(near, other_side, other_far), rows), :],
            dst_ref=lhs.at[n * rows : (n + 1) * rows, depth:],
            send_sem=rows_send.at[n],
            recv_sem=rows_recv.at[n],
            device_id=(dp, near),
            device_id_type=MESH,
        )

    def cols_copy(piece):
        return pltpu.make_async_remote_copy(
            src_ref=w_hbm.at[:, cols(dp, piece)],
            dst_ref=rhs.at[depth:, cols(dp, piece)],
            send_sem=cols_send.at[piece],
            recv_sem=cols_recv.at[piece, 0],
            device_id=(dp, near),
            device_id_type=MESH,
        )

    def relay(piece, origin, bit):
        window = rhs.at[depth:, cols(toggled(dp, origin), piece)]
        return pltpu.make_async_remote_copy(
            src_ref=window,
            dst_ref=window,
            send_sem=relay_sem.at[piece, origin, bits.index(bit)],
            recv_sem=cols_recv.at[piece, origin ^ bit],
            device_id=(flip(dp, bit), rank),
            device_id_type=MESH,
        )

    def cols_arrival(piece, origin):
        window = rhs.at[depth:, cols(toggled(dp, origin), piece)]
        return pltpu.make_async_remote_copy(
            src_ref=window,
            dst_ref=window,
            send_sem=cols_send.at[piece],
            recv_sem=cols_recv.at[piece, origin],
            device_id=(dp, near),
            device_id_type=MESH,
        )

    def onward(origin):
        return [bit for bit in bits if origin % (2 * bit) == 0]

    def side_copy(piece, origin):
        n = piece * replicas + origin
        return pltpu.make_async_remote_copy(
            src_ref=side_out.at[n],
            dst_ref=side_in.at[n],
            send_sem=side_send.at[n],
            recv_sem=side_recv.at[n],
            device_id=(dp, side),
            device_id_type=MESH,
        )

    def far_copy(piece, origin):
        n = piece * replicas + origin
        return pltpu.make_async_remote_copy(
            src_ref=far_out.at[n],
            dst_ref=far_in.at[n],
            send_sem=far_send.at[n],
            recv_sem=far_recv.at[n],
            device_id=(dp, far),
            device_id_type=MESH,
        )

    w_load = pltpu.make_async_copy(w_hbm, rhs.at[:depth, :], load_sem.at[0])
    x_loads = [
        pltpu.make_async_copy(
            x_hbm.at[pl.ds(place_of(rank, other_side, other_far), rows), :],
            lhs.at[n * rows : (n + 1) * rows, :depth],
            load_sem.at[1 + n],
        )
        for n, other_side, other_far in blocks
    ]
    w_load.start()
    for load in x_loads:
        load.start()
    for load in small:
        load.start()
    greet()
    for block in blocks[:2]:
        rows_copy(*block).start()
    cols_copy(0).start()
    for block in blocks[2:]:
        rows_copy(*block).start()
    for piece in range(1, PIECES):
        cols_copy(piece).start()
    for load in small:
        load.wait()
    routing(
        place_ref[...],
        chosen_ref[...],
        gates_ref[...],
        dp * lax.axis_size("tensor") + rank,
        rows,
        pick,
        combine_ref,
    )
    w_load.wait()
    for load in x_loads:
        load.wait()
    for block in blocks[:2]:
        rows_copy(*block).wait_recv()

    def begin(piece, origin):
        cols_arrival(piece, origin).wait_recv()
        for bit in onward(origin):
            relay(piece, origin, bit).start()
        here = cols(toggled(dp, origin), piece)
        side_out[piece * replicas + origin] = jnp.dot(
            lhs[: 2 * rows, :], rhs[:, here], preferred_element_type=jnp.float32
        ).astype(side_out.dtype)
        side_copy(piece, origin).start()

    def middle(piece, origin):
        n = piece * replicas + origin
        here = cols(toggled(dp, origin), piece)
        own = jnp.dot(lhs[2 * rows :, :], rhs[:, here], preferred_element_type=jnp.float32)
        side_copy(piece, origin).wait_recv()
        both = own + side_in[n].astype(jnp.float32)
        far_out[n] = both[rows:].astype(far_out.dtype)
        far_copy(piece, origin).start()
        state_ref[:, here] = both[:rows] + residual_ref[:, here].astype(jnp.float32)

    begin(0, 0)
    begin(0, 1)
    for block in blocks[2:]:
        rows_copy(*block).wait_recv()

    def step(piece, carry):
        for origin in range(replicas):
            if origin < 2:

                @pl.when(piece > 0)
                def _():
                    begin(piece, origin)
                    middle(piece - 1, origin + replicas - 2)

            else:
                begin(piece, origin)
                middle(piece, origin - 2)
        return carry

    lax.fori_loop(0, PIECES, step, 0)
    middle(PIECES - 1, replicas - 2)
    middle(PIECES - 1, replicas - 1)

    def finish(piece, squares):
        for origin in range(replicas):
            here = cols(toggled(dp, origin), piece)
            far_copy(piece, origin).wait_recv()
            state = state_ref[:, here] + far_in[piece * replicas + origin].astype(jnp.float32)
            state_ref[:, here] = state
            squares = squares + jnp.sum(state * state, axis=1, keepdims=True)
        return squares

    squares = lax.fori_loop(0, PIECES, finish, jnp.zeros((rows, 1), jnp.float32))
    scale = lax.rsqrt(squares / total + 1.0)
    slots = picked_ref.shape[0] * picked_ref.shape[1]
    selector = pick[...].reshape(slots, rows).astype(jnp.bfloat16)
    for lane in range(LANES):
        here = slice(lane * (total // LANES), (lane + 1) * (total // LANES))
        normed = (state_ref[:, here] * scale * norm_ref[:, here]).astype(jnp.bfloat16)
        chosen_rows = jnp.dot(selector, normed, preferred_element_type=jnp.float32)
        picked_ref[:, :, here] = chosen_rows.astype(picked_ref.dtype).reshape(
            picked_ref.shape[0], picked_ref.shape[1], total // LANES
        )
    def settle():
        for block in blocks:
            rows_copy(*block).wait_send()

        def drain(piece, carry):
            cols_copy(piece).wait_send()
            for origin in range(replicas):
                for bit in onward(origin):
                    relay(piece, origin, bit).wait_send()
                side_copy(piece, origin).wait_send()
                far_copy(piece, origin).wait_send()
            return carry

        lax.fori_loop(0, PIECES, drain, 0)

    return settle


class Place:
    def __init__(self, replicas, count):
        self.dp = lax.axis_index("dp")
        rank = lax.axis_index("tensor")
        self.odd = rank % 2
        self.per_row = count // 2
        self.pairs = replicas * self.per_row
        self.pair = self.dp * self.per_row + rank // 2
        self.partner = (self.dp, rank + 1 - 2 * self.odd)

    def device(self, pair):
        return (pair // self.per_row, 2 * (pair % self.per_row) + self.odd)

    def toggle(self, number):
        replicas = self.pairs // self.per_row
        near = number // replicas, number % replicas
        beyond = number - self.pairs // 2
        steps = self.per_row // 2
        far = steps + beyond % steps, beyond // steps
        is_far = number // (self.pairs // 2)
        row, column = (is_far * b + (1 - is_far) * a for a, b in zip(near, far))
        other = column * self.per_row + row
        total = 0
        bit = 1
        while bit < self.pairs:
            total = total + ((self.pair // bit + other // bit) % 2) * bit
            bit *= 2
        return total

    def greet(self):
        barrier = pltpu.get_barrier_semaphore()

        def signal(k, carry):
            target = self.device((self.pair + k) % self.pairs)
            pl.semaphore_signal(barrier, inc=1, device_id=target, device_id_type=MESH)
            return carry

        lax.fori_loop(1, self.pairs, signal, 0)
        pl.semaphore_signal(barrier, inc=1, device_id=self.partner, device_id_type=MESH)
        pl.semaphore_wait(barrier, self.pairs)


def loop(start, stop, body):
    def step(k, carry):
        body(k)
        return carry

    lax.fori_loop(start, stop, step, 0)


def experts_phase(
    at,
    group,
    greet,
    x_ref,
    state_ref,
    combine_ref,
    gate_hbm,
    up_hbm,
    down_hbm,
    out_ref,
    gate_w,
    up_w,
    down_w,
    received,
    result,
    part,
    returned,
    weight_sem,
    send_sem,
    pass_sem,
    recv_sem,
    cross_sem,
    part_sem,
    home_sem,
    done_sem,
):
    most, width = x_ref.shape[1:]
    rows = group * 2 * most
    groups = at.pairs // group

    def source(k):
        return at.toggle(k)

    def outward(k):
        target = at.toggle(k)
        return pltpu.make_async_remote_copy(
            src_ref=x_ref.at[target],
            dst_ref=received.at[k, at.odd],
            send_sem=send_sem.at[k],
            recv_sem=recv_sem.at[k, at.odd],
            device_id=at.device(target),
            device_id_type=MESH,
        )

    def sideways(k, side):
        return pltpu.make_async_remote_copy(
            src_ref=received.at[k, side],
            dst_ref=received.at[k, side],
            send_sem=pass_sem.at[k],
            recv_sem=recv_sem.at[k, side],
            device_id=at.partner,
            device_id_type=MESH,
        )

    def across(k):
        return pltpu.make_async_remote_copy(
            src_ref=result.at[k, 1 - at.odd],
            dst_ref=part.at[k],
            send_sem=cross_sem.at[k],
            recv_sem=part_sem.at[k],
            device_id=at.partner,
            device_id_type=MESH,
        )

    def home(k):
        return pltpu.make_async_remote_copy(
            src_ref=part.at[k],
            dst_ref=returned.at[at.pair],
            send_sem=home_sem.at[k],
            recv_sem=done_sem.at[at.pair],
            device_id=at.device(source(k)),
            device_id_type=MESH,
        )

    def forward(k):
        sideways(k, at.odd).wait_recv()
        sideways(k, at.odd).start()

    def add(k):
        across(k).wait_recv()
        part[k] = (
            part[k].astype(jnp.float32) + result[k, at.odd].astype(jnp.float32)
        ).astype(part.dtype)

    def add_and_send(k):
        add(k)
        home(k).start()

    loads = [
        pltpu.make_async_copy(hbm.at[0], vmem, weight_sem.at[n])
        for n, (hbm, vmem) in enumerate(((gate_hbm, gate_w), (up_hbm, up_w), (down_hbm, down_w)))
    ]
    if greet:
        for load in loads:
            load.start()
    own = pltpu.make_async_remote_copy(
        src_ref=x_ref.at[at.pair],
        dst_ref=received.at[0, at.odd],
        send_sem=pass_sem.at[0],
        recv_sem=recv_sem.at[0, at.odd],
        device_id=at.partner,
        device_id_type=MESH,
    )
    if greet:
        at.greet()
    else:
        for load in loads:
            load.start()

    def members(g):
        return max(g * group, 1), (g + 1) * group

    for g in SEND_ORDER:
        loop(*members(g), lambda k: outward(k).start())
    own.start()
    received[0, at.odd] = x_ref[at.pair]
    for g in range(AHEAD):
        loop(*members(g), forward)
    for load in loads:
        load.wait()
    contract = (((1,), (1,)), ((), ()))

    def step(g, carry):
        first = g * group
        start = first + AHEAD * group

        def forward_piece(piece):
            @pl.when(g + AHEAD < GROUPS)
            def _():
                cut = [start + n * group // PIECES for n in (piece, piece + 1)]
                loop(cut[0], cut[1], forward)

        loop(first, first + group, lambda k: sideways(k, 1 - at.odd).wait_recv())
        x = received[pl.ds(first, group)].reshape(rows, width)
        gate_part = lax.dot_general(x, gate_w[...], contract, preferred_element_type=jnp.float32)
        forward_piece(0)
        up_part = lax.dot_general(x, up_w[...], contract, preferred_element_type=jnp.float32)
        hidden = (gate_part / (1.0 + jnp.exp(-gate_part)) * up_part).astype(result.dtype)
        forward_piece(1)
        for piece in range(2):
            columns = slice(piece * (width // 2), (piece + 1) * (width // 2))
            y = jnp.dot(hidden, down_w[:, columns], preferred_element_type=jnp.float32)
            result[pl.ds(first, group), :, :, columns] = y.astype(result.dtype).reshape(
                group, 2, most, width // 2
            )
            forward_piece(2 + piece)

        for n, sets in ISSUE:
            @pl.when(g == n)
            def _():
                for h in sets:
                    crossing(h)

        return carry

    def crossing(g):
        loop(0, group, lambda k: across((g + 1) * group - 1 - k).start())

    def homeward(g):
        low, high = members(g)
        loop(0, high - low, lambda k: add_and_send(high - 1 - k))

    lax.fori_loop(0, GROUPS, step, 0)
    for g in HOME_ORDER:
        homeward(g)
    add(0)
    returned[at.pair] = part[0]

    def settle(k):
        pair = source(k)
        pltpu.make_async_remote_copy(
            src_ref=part.at[k],
            dst_ref=returned.at[pair],
            send_sem=home_sem.at[k],
            recv_sem=done_sem.at[pair],
            device_id=at.partner,
            device_id_type=MESH,
        ).wait_recv()

    loop(1, at.pairs, settle)
    combine = combine_ref[...].reshape(at.pairs * most, state_ref.shape[0])
    coarse = combine.astype(jnp.bfloat16)
    fine = (combine - coarse.astype(jnp.float32)).astype(jnp.bfloat16)
    over_slots = (((0,), (0,)), ((), ()))
    for piece in range(PIECES):
        columns = slice(piece * (width // PIECES), (piece + 1) * (width // PIECES))
        slots = returned[:, :, columns].reshape(at.pairs * most, width // PIECES)
        moe = lax.dot_general(
            coarse, slots, over_slots, preferred_element_type=jnp.float32
        ) + lax.dot_general(fine, slots, over_slots, preferred_element_type=jnp.float32)
        out_ref[:, columns] = (state_ref[:, columns] + moe).astype(out_ref.dtype)
    own.wait_send()
    across(0).wait_send()

    def drain(k):
        outward(k).wait_send()
        sideways(k, at.odd).wait_send()
        across(k).wait_send()
        home(k).wait_send()

    loop(1, at.pairs, drain)


def experts_kernel(replicas, count, group, *refs):
    experts_phase(Place(replicas, count), group, True, *refs)


def experts_scratch(pairs, most, width, hidden_units, dtype):
    weight = pltpu.VMEM((hidden_units, width), dtype)
    slots = pltpu.VMEM((pairs, most, width), dtype)
    sides = pltpu.VMEM((pairs, 2, most, width), dtype)
    return [
        weight,
        weight,
        weight,
        sides,
        sides,
        slots,
        slots,
        pltpu.SemaphoreType.DMA((3,)),
        pltpu.SemaphoreType.DMA((pairs,)),
        pltpu.SemaphoreType.DMA((pairs,)),
        pltpu.SemaphoreType.DMA((pairs, 2)),
        pltpu.SemaphoreType.DMA((pairs,)),
        pltpu.SemaphoreType.DMA((pairs,)),
        pltpu.SemaphoreType.DMA((pairs,)),
        pltpu.SemaphoreType.DMA((pairs,)),
    ]


def layer_kernel(replicas, count, group, *refs):
    x_hbm, w_hbm, residual, norm, chosen, gates, place, gate_hbm, up_hbm, down_hbm = refs[:10]
    out_ref, small_sem, state, picked, combine = refs[10:15]
    smalls, first, second = refs[15:20], refs[20:20 + FIRST], refs[20 + FIRST:]
    at = Place(replicas, count)
    small = [
        pltpu.make_async_copy(hbm, vmem, small_sem.at[n])
        for n, (hbm, vmem) in enumerate(zip((residual, norm, chosen, gates, place), smalls))
    ]
    settle = exchange_phase(
        replicas, at.greet, x_hbm, w_hbm, small, state, picked, combine, *smalls, *first
    )
    experts_phase(
        at, group, False, picked, state, combine, gate_hbm, up_hbm, down_hbm, out_ref, *second
    )
    settle()


def layer(x, w, residual, norm_gain, chosen, gates, place, w_gate, w_up, w_down, replicas, count):
    rows, columns = residual.shape
    depth = x.shape[1]
    width = columns // replicas // PIECES
    number = replicas * PIECES
    experts, capacity = chosen.shape
    most = 2 * capacity // (replicas * count)
    hidden_units = w_gate.shape[1]
    half = jnp.bfloat16
    dma = pltpu.SemaphoreType.DMA
    arrays = (x, w, residual, norm_gain[None, :], chosen, gates, place[None, :])
    first = [
        pltpu.VMEM((4 * rows, 2 * depth), half),
        pltpu.VMEM((2 * depth, columns), half),
        pltpu.VMEM((number, 2 * rows, width), half),
        pltpu.VMEM((number, 2 * rows, width), half),
        pltpu.VMEM((number, rows, width), half),
        pltpu.VMEM((number, rows, width), half),
        pltpu.VMEM((experts, most, rows), jnp.float32),
        dma((5,)),
        dma((4,)),
        dma((4,)),
        dma((PIECES,)),
        dma((PIECES, replicas)),
        dma((PIECES, replicas, replicas.bit_length() - 1)),
        dma((number,)),
        dma((number,)),
        dma((number,)),
        dma((number,)),
    ]
    return pl.pallas_call(
        functools.partial(layer_kernel, replicas, count, experts // GROUPS),
        out_shape=jax.ShapeDtypeStruct((rows, columns), half),
        in_specs=[pl.BlockSpec(memory_space=pltpu.HBM)] * 10,
        out_specs=pl.BlockSpec(memory_space=pltpu.VMEM),
        scratch_shapes=[
            dma((5,)),
            pltpu.VMEM((rows, columns), jnp.float32),
            pltpu.VMEM((experts, most, columns), half),
            pltpu.VMEM((experts, most, rows), jnp.float32),
        ]
        + [pltpu.VMEM(array.shape, array.dtype) for array in arrays[2:]]
        + first
        + experts_scratch(experts, most, columns, hidden_units, half),
        compiler_params=pltpu.CompilerParams(
            collective_id=2, has_side_effects=True, vmem_limit_bytes=LIMIT * 1024 * 1024
        ),
    )(*arrays, w_gate, w_up, w_down)


def experts_layer(x, state, combine, w_gate, w_up, w_down, replicas, count):
    pairs, most, width = x.shape
    group = pairs // GROUPS
    hidden_units = w_gate.shape[1]
    whole = pl.BlockSpec(memory_space=pltpu.VMEM)
    return pl.pallas_call(
        functools.partial(experts_kernel, replicas, count, group),
        out_shape=jax.ShapeDtypeStruct(state.shape, x.dtype),
        in_specs=[whole] * 3 + [pl.BlockSpec(memory_space=pl.ANY)] * 3,
        out_specs=whole,
        scratch_shapes=experts_scratch(pairs, most, width, hidden_units, x.dtype),
        compiler_params=pltpu.CompilerParams(
            collective_id=1, has_side_effects=True, vmem_limit_bytes=44 * 1024 * 1024
        ),
    )(x, state, combine, w_gate, w_up, w_down)


def on_device(
    head_outputs, out_weight, residual, norm_gain, chosen, gates, place, w_gate, w_up, w_down
):
    count = lax.axis_size("tensor")
    replicas = lax.axis_size("dp")
    routed = (head_outputs, out_weight, residual, norm_gain, chosen, gates, place)
    if count == 8 and replicas >= 4:
        return layer(*routed, w_gate, w_up, w_down, replicas, count)
    state, picked, combine = project(*routed, replicas, count)
    experts, most = combine.shape[:2]
    picked = picked.reshape(experts, most, residual.shape[1])
    return experts_layer(picked, state, combine, w_gate, w_up, w_down, replicas, count)


def solution(mesh):
    return jax.shard_map(
        on_device,
        mesh=mesh,
        in_specs=(
            P("dp", "tensor"),
            P("tensor", None),
            P(("dp", "tensor"), None),
            P(),
            P(),
            P(),
            P(),
            P(("dp", "tensor"), None, None),
            P(("dp", "tensor"), None, None),
            P(("dp", "tensor"), None, None),
        ),
        out_specs=P(("dp", "tensor"), None),
        check_vma=False,
    )
```

```python
import functools

import jax
import jax.numpy as jnp
from jax import lax
from jax.experimental import pallas as pl
from jax.experimental.pallas import tpu as pltpu
from jax.sharding import PartitionSpec as P

MESH = pl.DeviceIdType.MESH
LANES = 4
PIECES = 4
GROUPS = 4
FIRST = 17
LIMIT = 58
LAG = 2
AHEAD = 2
SEND_ORDER = (1, 2, 3, 0)
HOME_ORDER = (2, 1, 3, 0)
ISSUE = ((2, (2, 1)), (3, (3, 0)))


def ring_rank(position, count):
    upper = position // (count // 2)
    return (1 - upper) * 2 * position + upper * (2 * (count - 1 - position) + 1)


def routing(place, chosen, gates, my_index, row_count, pick, gain_ref):
    experts, capacity = chosen.shape
    most = pick.shape[1]
    pair_ids = lax.broadcasted_iota(jnp.int32, (experts, experts), 0)
    pair_map = (place == pair_ids).astype(jnp.float32)
    chosen_pair = jnp.dot(
        pair_map,
        chosen.astype(jnp.float32),
        precision=lax.Precision.HIGHEST,
        preferred_element_type=jnp.float32,
    ).astype(jnp.int32)
    gates_pair = jnp.dot(
        pair_map, gates, precision=lax.Precision.HIGHEST, preferred_element_type=jnp.float32
    )
    local_row = chosen_pair - my_index * row_count
    is_mine = (local_row >= 0) & (local_row < row_count)
    before = lax.broadcasted_iota(jnp.int32, (capacity, capacity), 0)
    after = lax.broadcasted_iota(jnp.int32, (capacity, capacity), 1)
    slot_rank = jnp.dot(
        is_mine.astype(jnp.float32).astype(jnp.bfloat16),
        (before < after).astype(jnp.float32).astype(jnp.bfloat16),
        preferred_element_type=jnp.float32,
    ).astype(jnp.int32)
    row_ids = lax.broadcasted_iota(jnp.int32, (experts, row_count), 1)
    shifted = (local_row + 1).astype(jnp.float32)
    for m in range(most):
        match = is_mine & (slot_rank == m)
        target = jnp.sum(jnp.where(match, shifted, 0.0), axis=1, keepdims=True)
        gate = jnp.sum(jnp.where(match, gates_pair, 0.0), axis=1, keepdims=True)
        hit = target.astype(jnp.int32) - 1 == row_ids
        pick[:, m, :] = hit.astype(jnp.float32)
        gain_ref[:, m, :] = jnp.where(hit, gate, 0.0)


def project_kernel(
    replicas,
    count,
    x_hbm,
    w_hbm,
    residual_ref,
    norm_ref,
    chosen_ref,
    gates_ref,
    place_ref,
    state_ref,
    picked_ref,
    combine_ref,
    x_ref,
    w_ref,
    held,
    term,
    pick,
    load_sem,
    send_sem,
    recv_sem,
):
    dp = lax.axis_index("dp")
    rank = lax.axis_index("tensor")
    odd = rank % 2
    half = rank // 2
    here = (1 - odd) * half + odd * (count - 1 - half)
    right = ring_rank((here + 1) % count, count)
    left = ring_rank((here + count - 1) % count, count)
    rows = state_ref.shape[0]
    width = state_ref.shape[1] // LANES
    order = [lane for k in range(LANES // 2) for lane in (k, LANES // 2 + k)]

    def columns(lane):
        return slice(lane * width, (lane + 1) * width)

    loads = {
        lane: pltpu.make_async_copy(
            w_hbm.at[:, columns(lane)], w_ref.at[:, columns(lane)], load_sem.at[lane]
        )
        for lane in order
    }
    x_load = pltpu.make_async_copy(x_hbm, x_ref, load_sem.at[LANES])
    loads[order[0]].start()
    x_load.start()
    for lane in order[1:]:
        loads[lane].start()

    def own_term(lane, block):
        start = pl.multiple_of(ring_rank(block, count) * rows, rows)
        return jnp.dot(
            x_ref[pl.ds(start, rows), :],
            w_ref[:, columns(lane)],
            preferred_element_type=jnp.float32,
        )

    def block_of(lane, slot):
        if lane < LANES // 2:
            return (here + 2 * count - 1 - slot) % count
        return (here + 1 + slot) % count

    def copy(lane, slot):
        return pltpu.make_async_remote_copy(
            src_ref=held.at[lane, slot],
            dst_ref=held.at[lane, slot + 1],
            send_sem=send_sem.at[lane, slot],
            recv_sem=recv_sem.at[lane, slot + 1],
            device_id=(dp, right if lane < LANES // 2 else left),
            device_id_type=MESH,
        )

    def arrival(lane, slot):
        return pltpu.make_async_remote_copy(
            src_ref=held.at[lane, slot],
            dst_ref=held.at[lane, slot],
            send_sem=send_sem.at[lane, slot],
            recv_sem=recv_sem.at[lane, slot],
            device_id=(dp, right if lane < LANES // 2 else left),
            device_id_type=MESH,
        )

    barrier = pltpu.get_barrier_semaphore()
    for neighbour in (left, right):
        pl.semaphore_signal(barrier, inc=1, device_id=(dp, neighbour), device_id_type=MESH)
    x_load.wait()
    for n, lane in enumerate(order):
        loads[lane].wait()
        held[lane, 0] = own_term(lane, block_of(lane, 0)).astype(held.dtype)
        if n == 0:
            pl.semaphore_wait(barrier, 2)
        copy(lane, 0).start()

    routing(
        place_ref[...],
        chosen_ref[...],
        gates_ref[...],
        dp * count + rank,
        rows,
        pick,
        combine_ref,
    )

    def step(slot, carry):
        for lane in order:
            term[lane] = own_term(lane, block_of(lane, slot))
        for lane in order:
            arrival(lane, slot).wait_recv()
            held[lane, slot] = (held[lane, slot].astype(jnp.float32) + term[lane]).astype(held.dtype)
            copy(lane, slot).start()
        return carry

    lax.fori_loop(1, count - 1, step, 0)
    last = count - 1
    for lane in order:
        term[lane] = own_term(lane, block_of(lane, last)) + residual_ref[:, columns(lane)].astype(
            jnp.float32
        )
    total = jnp.zeros((rows, 1), jnp.float32)
    for lane in order:
        arrival(lane, last).wait_recv()
        state = held[lane, last].astype(jnp.float32) + term[lane]
        state_ref[:, columns(lane)] = state
        total = total + jnp.sum(state * state, axis=1, keepdims=True)
    scale = lax.rsqrt(total / (LANES * width) + 1.0)
    selector = pick[...].reshape(picked_ref.shape[0], rows).astype(jnp.bfloat16)
    for lane in order:
        normed = (state_ref[:, columns(lane)] * scale * norm_ref[:, columns(lane)]).astype(
            jnp.bfloat16
        )
        picked_ref[:, columns(lane)] = jnp.dot(
            selector, normed, preferred_element_type=jnp.float32
        ).astype(picked_ref.dtype)

    def drain(slot, carry):
        for lane in order:
            copy(lane, slot).wait_send()
        return carry

    lax.fori_loop(0, count - 1, drain, 0)


def project(x, w, residual, norm_gain, chosen, gates, place, replicas, count):
    rows, columns = residual.shape
    width = columns // LANES
    experts, capacity = chosen.shape
    most = 2 * capacity // (replicas * count)
    whole = pl.BlockSpec(memory_space=pltpu.VMEM)
    outside = pl.BlockSpec(memory_space=pl.ANY)
    return pl.pallas_call(
        functools.partial(project_kernel, replicas, count),
        out_shape=(
            jax.ShapeDtypeStruct((rows, columns), jnp.float32),
            jax.ShapeDtypeStruct((experts * most, columns), jnp.bfloat16),
            jax.ShapeDtypeStruct((experts, most, rows), jnp.float32),
        ),
        in_specs=[outside, outside] + [whole] * 5,
        out_specs=(whole, whole, whole),
        scratch_shapes=[
            pltpu.VMEM(x.shape, x.dtype),
            pltpu.VMEM(w.shape, w.dtype),
            pltpu.VMEM((LANES, count, rows, width), jnp.bfloat16),
            pltpu.VMEM((LANES, rows, width), jnp.float32),
            pltpu.VMEM((experts, most, rows), jnp.float32),
            pltpu.SemaphoreType.DMA((LANES + 1,)),
            pltpu.SemaphoreType.DMA((LANES, count)),
            pltpu.SemaphoreType.DMA((LANES, count)),
        ],
        compiler_params=pltpu.CompilerParams(
            collective_id=0, has_side_effects=True, vmem_limit_bytes=44 * 1024 * 1024
        ),
    )(x, w, residual, norm_gain[None, :], chosen, gates, place[None, :])


def flip(value, bit):
    return value + bit - 2 * bit * ((value // bit) % 2)


def toggled(value, mask):
    bit = 1
    while bit <= mask:
        if mask & bit:
            value = flip(value, bit)
        bit *= 2
    return value


def exchange_phase(
    replicas,
    greet,
    meanwhile,
    x_hbm,
    w_hbm,
    small,
    state_ref,
    picked_ref,
    combine_ref,
    residual_ref,
    norm_ref,
    chosen_ref,
    gates_ref,
    place_ref,
    lhs,
    rhs,
    side_out,
    side_in,
    far_out,
    far_in,
    pick,
    load_sem,
    rows_send,
    rows_recv,
    cols_send,
    cols_recv,
    relay_sem,
    side_send,
    side_recv,
    far_send,
    far_recv,
):
    dp = lax.axis_index("dp")
    rank = lax.axis_index("tensor")
    near, side, far = flip(rank, 2), flip(rank, 1), flip(rank, 4)
    rows, total = state_ref.shape
    depth = x_hbm.shape[1]
    share = total // replicas
    width = share // PIECES
    bits = [1 << n for n in range(replicas.bit_length() - 1)]
    blocks = [(n, 1 - n // 2, n % 2) for n in range(4)]

    def place_of(owner, other_side, other_far):
        mask = other_side + 4 * other_far
        return pl.multiple_of(toggled(owner, mask) * rows, rows)

    def cols(origin, piece):
        return pl.ds(pl.multiple_of(origin * share + piece * width, width), width)

    def rows_copy(n, other_side, other_far):
        return pltpu.make_async_remote_copy(
            src_ref=x_hbm.at[pl.ds(place_of(near, other_side, other_far), rows), :],
            dst_ref=lhs.at[n * rows : (n + 1) * rows, depth:],
            send_sem=rows_send.at[n],
            recv_sem=rows_recv.at[n],
            device_id=(dp, near),
            device_id_type=MESH,
        )

    def cols_copy(piece):
        return pltpu.make_async_remote_copy(
            src_ref=w_hbm.at[:, cols(dp, piece)],
            dst_ref=rhs.at[depth:, cols(dp, piece)],
            send_sem=cols_send.at[piece],
            recv_sem=cols_recv.at[piece, 0],
            device_id=(dp, near),
            device_id_type=MESH,
        )

    def relay(piece, origin, bit):
        window = rhs.at[depth:, cols(toggled(dp, origin), piece)]
        return pltpu.make_async_remote_copy(
            src_ref=window,
            dst_ref=window,
            send_sem=relay_sem.at[piece, origin, bits.index(bit)],
            recv_sem=cols_recv.at[piece, origin ^ bit],
            device_id=(flip(dp, bit), rank),
            device_id_type=MESH,
        )

    def cols_arrival(piece, origin):
        window = rhs.at[depth:, cols(toggled(dp, origin), piece)]
        return pltpu.make_async_remote_copy(
            src_ref=window,
            dst_ref=window,
            send_sem=cols_send.at[piece],
            recv_sem=cols_recv.at[piece, origin],
            device_id=(dp, near),
            device_id_type=MESH,
        )

    def onward(origin):
        return [bit for bit in bits if origin % (2 * bit) == 0]

    def side_copy(piece, origin):
        n = piece * replicas + origin
        return pltpu.make_async_remote_copy(
            src_ref=side_out.at[n],
            dst_ref=side_in.at[n],
            send_sem=side_send.at[n],
            recv_sem=side_recv.at[n],
            device_id=(dp, side),
            device_id_type=MESH,
        )

    def far_copy(piece, origin):
        n = piece * replicas + origin
        return pltpu.make_async_remote_copy(
            src_ref=far_out.at[n],
            dst_ref=far_in.at[n],
            send_sem=far_send.at[n],
            recv_sem=far_recv.at[n],
            device_id=(dp, far),
            device_id_type=MESH,
        )

    w_load = pltpu.make_async_copy(w_hbm, rhs.at[:depth, :], load_sem.at[0])
    x_loads = [
        pltpu.make_async_copy(
            x_hbm.at[pl.ds(place_of(rank, other_side, other_far), rows), :],
            lhs.at[n * rows : (n + 1) * rows, :depth],
            load_sem.at[1 + n],
        )
        for n, other_side, other_far in blocks
    ]
    w_load.start()
    for load in x_loads:
        load.start()
    for load in small:
        load.start()
    greet()
    for block in blocks[:2]:
        rows_copy(*block).start()
    cols_copy(0).start()
    for block in blocks[2:]:
        rows_copy(*block).start()
    cols_copy(1).start()
    meanwhile()
    for load in small:
        load.wait()
    routing(
        place_ref[...],
        chosen_ref[...],
        gates_ref[...],
        dp * lax.axis_size("tensor") + rank,
        rows,
        pick,
        combine_ref,
    )
    w_load.wait()
    for load in x_loads:
        load.wait()
    for block in blocks[:2]:
        rows_copy(*block).wait_recv()

    def pass_on(piece, origin):
        cols_arrival(piece, origin).wait_recv()
        for bit in onward(origin):
            relay(piece, origin, bit).start()
        if origin == 0 and isinstance(piece, int) is False or origin == 0 and piece == 1:

            @pl.when(piece + 1 < PIECES)
            def _():
                cols_copy(piece + 1).start()

    def begin(piece, origin):
        if origin > 0:
            pass_on(piece, origin)
        here = cols(toggled(dp, origin), piece)
        side_out[piece * replicas + origin] = jnp.dot(
            lhs[: 2 * rows, :], rhs[:, here], preferred_element_type=jnp.float32
        ).astype(side_out.dtype)
        side_copy(piece, origin).start()

    def middle(piece, origin):
        n = piece * replicas + origin
        here = cols(toggled(dp, origin), piece)
        own = jnp.dot(lhs[2 * rows :, :], rhs[:, here], preferred_element_type=jnp.float32)
        side_copy(piece, origin).wait_recv()
        both = own + side_in[n].astype(jnp.float32)
        far_out[n] = both[rows:].astype(far_out.dtype)
        far_copy(piece, origin).start()
        state_ref[:, here] = both[:rows] + residual_ref[:, here].astype(jnp.float32)

    pass_on(0, 0)
    for origin in range(LAG):
        begin(0, origin)
    for block in blocks[2:]:
        rows_copy(*block).wait_recv()

    def step(piece, carry):
        @pl.when(piece == 1)
        def _():
            pass_on(1, 0)

        for origin in range(replicas):
            if origin == 2:

                @pl.when((piece > 0) & (piece + 1 < PIECES))
                def _():
                    pass_on(piece + 1, 0)

            if origin < LAG:

                @pl.when(piece > 0)
                def _():
                    begin(piece, origin)
                    middle(piece - 1, origin + replicas - LAG)

            else:
                begin(piece, origin)
                middle(piece, origin - LAG)
        return carry

    lax.fori_loop(0, PIECES, step, 0)
    for origin in range(replicas - LAG, replicas):
        middle(PIECES - 1, origin)

    def finish(piece, squares):
        for origin in range(replicas):
            here = cols(toggled(dp, origin), piece)
            far_copy(piece, origin).wait_recv()
            state = state_ref[:, here] + far_in[piece * replicas + origin].astype(jnp.float32)
            state_ref[:, here] = state
            squares = squares + jnp.sum(state * state, axis=1, keepdims=True)
        return squares

    squares = lax.fori_loop(0, PIECES, finish, jnp.zeros((rows, 1), jnp.float32))
    scale = lax.rsqrt(squares / total + 1.0)
    slots = picked_ref.shape[0] * picked_ref.shape[1]
    selector = pick[...].reshape(slots, rows).astype(jnp.bfloat16)
    for lane in range(LANES):
        here = slice(lane * (total // LANES), (lane + 1) * (total // LANES))
        normed = (state_ref[:, here] * scale * norm_ref[:, here]).astype(jnp.bfloat16)
        chosen_rows = jnp.dot(selector, normed, preferred_element_type=jnp.float32)
        picked_ref[:, :, here] = chosen_rows.astype(picked_ref.dtype).reshape(
            picked_ref.shape[0], picked_ref.shape[1], total // LANES
        )
    def settle():
        for block in blocks:
            rows_copy(*block).wait_send()

        def drain(piece, carry):
            cols_copy(piece).wait_send()
            for origin in range(replicas):
                for bit in onward(origin):
                    relay(piece, origin, bit).wait_send()
                side_copy(piece, origin).wait_send()
                far_copy(piece, origin).wait_send()
            return carry

        lax.fori_loop(0, PIECES, drain, 0)

    return settle


class Place:
    def __init__(self, replicas, count):
        self.dp = lax.axis_index("dp")
        rank = lax.axis_index("tensor")
        self.odd = rank % 2
        self.per_row = count // 2
        self.pairs = replicas * self.per_row
        self.pair = self.dp * self.per_row + rank // 2
        self.partner = (self.dp, rank + 1 - 2 * self.odd)

    def device(self, pair):
        return (pair // self.per_row, 2 * (pair % self.per_row) + self.odd)

    def toggle(self, number):
        replicas = self.pairs // self.per_row
        near = number // replicas, number % replicas
        beyond = number - self.pairs // 2
        steps = self.per_row // 2
        far = steps + beyond % steps, beyond // steps
        is_far = number // (self.pairs // 2)
        row, column = (is_far * b + (1 - is_far) * a for a, b in zip(near, far))
        other = column * self.per_row + row
        total = 0
        bit = 1
        while bit < self.pairs:
            total = total + ((self.pair // bit + other // bit) % 2) * bit
            bit *= 2
        return total

    def greet(self):
        barrier = pltpu.get_barrier_semaphore()

        def signal(k, carry):
            target = self.device((self.pair + k) % self.pairs)
            pl.semaphore_signal(barrier, inc=1, device_id=target, device_id_type=MESH)
            return carry

        lax.fori_loop(1, self.pairs, signal, 0)
        pl.semaphore_signal(barrier, inc=1, device_id=self.partner, device_id_type=MESH)
        pl.semaphore_wait(barrier, self.pairs)


def loop(start, stop, body):
    def step(k, carry):
        body(k)
        return carry

    lax.fori_loop(start, stop, step, 0)


def weight_loads(gate_hbm, up_hbm, down_hbm, gate_w, up_w, down_w, weight_sem):
    return [
        pltpu.make_async_copy(hbm.at[0], vmem, weight_sem.at[n])
        for n, (hbm, vmem) in enumerate(((gate_hbm, gate_w), (up_hbm, up_w), (down_hbm, down_w)))
    ]


def experts_phase(
    at,
    group,
    greet,
    x_ref,
    state_ref,
    combine_ref,
    gate_hbm,
    up_hbm,
    down_hbm,
    out_ref,
    gate_w,
    up_w,
    down_w,
    received,
    result,
    part,
    returned,
    weight_sem,
    send_sem,
    pass_sem,
    recv_sem,
    cross_sem,
    part_sem,
    home_sem,
    done_sem,
):
    most, width = x_ref.shape[1:]
    rows = group * 2 * most
    groups = at.pairs // group

    def source(k):
        return at.toggle(k)

    def outward(k):
        target = at.toggle(k)
        return pltpu.make_async_remote_copy(
            src_ref=x_ref.at[target],
            dst_ref=received.at[k, at.odd],
            send_sem=send_sem.at[k],
            recv_sem=recv_sem.at[k, at.odd],
            device_id=at.device(target),
            device_id_type=MESH,
        )

    def sideways(k, side):
        return pltpu.make_async_remote_copy(
            src_ref=received.at[k, side],
            dst_ref=received.at[k, side],
            send_sem=pass_sem.at[k],
            recv_sem=recv_sem.at[k, side],
            device_id=at.partner,
            device_id_type=MESH,
        )

    def across(k):
        return pltpu.make_async_remote_copy(
            src_ref=result.at[k, 1 - at.odd],
            dst_ref=part.at[k],
            send_sem=cross_sem.at[k],
            recv_sem=part_sem.at[k],
            device_id=at.partner,
            device_id_type=MESH,
        )

    def home(k):
        return pltpu.make_async_remote_copy(
            src_ref=part.at[k],
            dst_ref=returned.at[at.pair],
            send_sem=home_sem.at[k],
            recv_sem=done_sem.at[at.pair],
            device_id=at.device(source(k)),
            device_id_type=MESH,
        )

    def forward(k):
        sideways(k, at.odd).wait_recv()
        sideways(k, at.odd).start()

    def add(k):
        across(k).wait_recv()
        part[k] = (
            part[k].astype(jnp.float32) + result[k, at.odd].astype(jnp.float32)
        ).astype(part.dtype)

    def add_and_send(k):
        add(k)
        home(k).start()

    loads = weight_loads(gate_hbm, up_hbm, down_hbm, gate_w, up_w, down_w, weight_sem)
    if greet:
        for load in loads:
            load.start()
    own = pltpu.make_async_remote_copy(
        src_ref=x_ref.at[at.pair],
        dst_ref=received.at[0, at.odd],
        send_sem=pass_sem.at[0],
        recv_sem=recv_sem.at[0, at.odd],
        device_id=at.partner,
        device_id_type=MESH,
    )
    if greet:
        at.greet()

    def members(g):
        return max(g * group, 1), (g + 1) * group

    for g in SEND_ORDER:
        loop(*members(g), lambda k: outward(k).start())
    own.start()
    received[0, at.odd] = x_ref[at.pair]
    for g in range(AHEAD):
        loop(*members(g), forward)
    for load in loads:
        load.wait()
    contract = (((1,), (1,)), ((), ()))

    def step(g, carry):
        first = g * group

        def forward_piece(piece):
            @pl.when(g == 0)
            def _():
                cut = [n * group // PIECES for n in (piece, piece + 1)]
                loop(AHEAD * group + cut[0], AHEAD * group + cut[1], forward)

            @pl.when((g > 0) & (g < GROUPS - 1))
            def _():
                turn = (g - 1) * PIECES + piece
                cut = [n * group // (2 * PIECES) for n in (turn, turn + 1)]
                loop((AHEAD + 1) * group + cut[0], (AHEAD + 1) * group + cut[1], forward)

        loop(first, first + group, lambda k: sideways(k, 1 - at.odd).wait_recv())
        x = received[pl.ds(first, group)].reshape(rows, width)
        gate_part = lax.dot_general(x, gate_w[...], contract, preferred_element_type=jnp.float32)
        forward_piece(0)
        up_part = lax.dot_general(x, up_w[...], contract, preferred_element_type=jnp.float32)
        hidden = (gate_part / (1.0 + jnp.exp(-gate_part)) * up_part).astype(result.dtype)
        forward_piece(1)
        for piece in range(2):
            columns = slice(piece * (width // 2), (piece + 1) * (width // 2))
            y = jnp.dot(hidden, down_w[:, columns], preferred_element_type=jnp.float32)
            result[pl.ds(first, group), :, :, columns] = y.astype(result.dtype).reshape(
                group, 2, most, width // 2
            )
            forward_piece(2 + piece)

        for n, sets in ISSUE:
            @pl.when(g == n)
            def _():
                for h in sets:
                    crossing(h)

        return carry

    def crossing(g):
        loop(0, group, lambda k: across((g + 1) * group - 1 - k).start())

    def homeward(g):
        low, high = members(g)
        loop(0, high - low, lambda k: add_and_send(high - 1 - k))

    lax.fori_loop(0, GROUPS, step, 0)
    for g in HOME_ORDER:
        homeward(g)
    add(0)
    returned[at.pair] = part[0]

    def settle(k):
        pair = source(k)
        pltpu.make_async_remote_copy(
            src_ref=part.at[k],
            dst_ref=returned.at[pair],
            send_sem=home_sem.at[k],
            recv_sem=done_sem.at[pair],
            device_id=at.partner,
            device_id_type=MESH,
        ).wait_recv()

    loop(1, at.pairs, settle)
    combine = combine_ref[...].reshape(at.pairs * most, state_ref.shape[0])
    coarse = combine.astype(jnp.bfloat16)
    fine = (combine - coarse.astype(jnp.float32)).astype(jnp.bfloat16)
    over_slots = (((0,), (0,)), ((), ()))
    for piece in range(PIECES):
        columns = slice(piece * (width // PIECES), (piece + 1) * (width // PIECES))
        slots = returned[:, :, columns].reshape(at.pairs * most, width // PIECES)
        moe = lax.dot_general(
            coarse, slots, over_slots, preferred_element_type=jnp.float32
        ) + lax.dot_general(fine, slots, over_slots, preferred_element_type=jnp.float32)
        out_ref[:, columns] = (state_ref[:, columns] + moe).astype(out_ref.dtype)
    own.wait_send()
    across(0).wait_send()

    def drain(k):
        outward(k).wait_send()
        sideways(k, at.odd).wait_send()
        across(k).wait_send()
        home(k).wait_send()

    loop(1, at.pairs, drain)


def experts_kernel(replicas, count, group, *refs):
    experts_phase(Place(replicas, count), group, True, *refs)


def experts_scratch(pairs, most, width, hidden_units, dtype):
    weight = pltpu.VMEM((hidden_units, width), dtype)
    slots = pltpu.VMEM((pairs, most, width), dtype)
    sides = pltpu.VMEM((pairs, 2, most, width), dtype)
    return [
        weight,
        weight,
        weight,
        sides,
        sides,
        slots,
        slots,
        pltpu.SemaphoreType.DMA((3,)),
        pltpu.SemaphoreType.DMA((pairs,)),
        pltpu.SemaphoreType.DMA((pairs,)),
        pltpu.SemaphoreType.DMA((pairs, 2)),
        pltpu.SemaphoreType.DMA((pairs,)),
        pltpu.SemaphoreType.DMA((pairs,)),
        pltpu.SemaphoreType.DMA((pairs,)),
        pltpu.SemaphoreType.DMA((pairs,)),
    ]


def layer_kernel(replicas, count, group, *refs):
    x_hbm, w_hbm, residual, norm, chosen, gates, place, gate_hbm, up_hbm, down_hbm = refs[:10]
    out_ref, small_sem, state, picked, combine = refs[10:15]
    smalls, first, second = refs[15:20], refs[20:20 + FIRST], refs[20 + FIRST:]
    at = Place(replicas, count)
    small = [
        pltpu.make_async_copy(hbm, vmem, small_sem.at[n])
        for n, (hbm, vmem) in enumerate(zip((residual, norm, chosen, gates, place), smalls))
    ]

    def meanwhile():
        for load in weight_loads(gate_hbm, up_hbm, down_hbm, *second[:3], second[7]):
            load.start()

    settle = exchange_phase(
        replicas, at.greet, meanwhile, x_hbm, w_hbm, small, state, picked, combine, *smalls, *first
    )
    experts_phase(
        at, group, False, picked, state, combine, gate_hbm, up_hbm, down_hbm, out_ref, *second
    )
    settle()


def layer(x, w, residual, norm_gain, chosen, gates, place, w_gate, w_up, w_down, replicas, count):
    rows, columns = residual.shape
    depth = x.shape[1]
    width = columns // replicas // PIECES
    number = replicas * PIECES
    experts, capacity = chosen.shape
    most = 2 * capacity // (replicas * count)
    hidden_units = w_gate.shape[1]
    half = jnp.bfloat16
    dma = pltpu.SemaphoreType.DMA
    arrays = (x, w, residual, norm_gain[None, :], chosen, gates, place[None, :])
    first = [
        pltpu.VMEM((4 * rows, 2 * depth), half),
        pltpu.VMEM((2 * depth, columns), half),
        pltpu.VMEM((number, 2 * rows, width), half),
        pltpu.VMEM((number, 2 * rows, width), half),
        pltpu.VMEM((number, rows, width), half),
        pltpu.VMEM((number, rows, width), half),
        pltpu.VMEM((experts, most, rows), jnp.float32),
        dma((5,)),
        dma((4,)),
        dma((4,)),
        dma((PIECES,)),
        dma((PIECES, replicas)),
        dma((PIECES, replicas, replicas.bit_length() - 1)),
        dma((number,)),
        dma((number,)),
        dma((number,)),
        dma((number,)),
    ]
    return pl.pallas_call(
        functools.partial(layer_kernel, replicas, count, experts // GROUPS),
        out_shape=jax.ShapeDtypeStruct((rows, columns), half),
        in_specs=[pl.BlockSpec(memory_space=pltpu.HBM)] * 10,
        out_specs=pl.BlockSpec(memory_space=pltpu.VMEM),
        scratch_shapes=[
            dma((5,)),
            pltpu.VMEM((rows, columns), jnp.float32),
            pltpu.VMEM((experts, most, columns), half),
            pltpu.VMEM((experts, most, rows), jnp.float32),
        ]
        + [pltpu.VMEM(array.shape, array.dtype) for array in arrays[2:]]
        + first
        + experts_scratch(experts, most, columns, hidden_units, half),
        compiler_params=pltpu.CompilerParams(
            collective_id=2, has_side_effects=True, vmem_limit_bytes=LIMIT * 1024 * 1024
        ),
    )(*arrays, w_gate, w_up, w_down)


def experts_layer(x, state, combine, w_gate, w_up, w_down, replicas, count):
    pairs, most, width = x.shape
    group = pairs // GROUPS
    hidden_units = w_gate.shape[1]
    whole = pl.BlockSpec(memory_space=pltpu.VMEM)
    return pl.pallas_call(
        functools.partial(experts_kernel, replicas, count, group),
        out_shape=jax.ShapeDtypeStruct(state.shape, x.dtype),
        in_specs=[whole] * 3 + [pl.BlockSpec(memory_space=pl.ANY)] * 3,
        out_specs=whole,
        scratch_shapes=experts_scratch(pairs, most, width, hidden_units, x.dtype),
        compiler_params=pltpu.CompilerParams(
            collective_id=1, has_side_effects=True, vmem_limit_bytes=44 * 1024 * 1024
        ),
    )(x, state, combine, w_gate, w_up, w_down)


def on_device(
    head_outputs, out_weight, residual, norm_gain, chosen, gates, place, w_gate, w_up, w_down
):
    count = lax.axis_size("tensor")
    replicas = lax.axis_size("dp")
    routed = (head_outputs, out_weight, residual, norm_gain, chosen, gates, place)
    if count == 8 and replicas >= 4:
        return layer(*routed, w_gate, w_up, w_down, replicas, count)
    state, picked, combine = project(*routed, replicas, count)
    experts, most = combine.shape[:2]
    picked = picked.reshape(experts, most, residual.shape[1])
    return experts_layer(picked, state, combine, w_gate, w_up, w_down, replicas, count)


def solution(mesh):
    return jax.shard_map(
        on_device,
        mesh=mesh,
        in_specs=(
            P("dp", "tensor"),
            P("tensor", None),
            P(("dp", "tensor"), None),
            P(),
            P(),
            P(),
            P(),
            P(("dp", "tensor"), None, None),
            P(("dp", "tensor"), None, None),
            P(("dp", "tensor"), None, None),
        ),
        out_specs=P(("dp", "tensor"), None),
        check_vma=False,
    )
```
